32 devices in a mesh: data: 1 (over z), wg: 32 (over y, x, core).
Axes of the slice: x: 4, y: 4, z: 1, core: 2. Of those that a mesh axis runs over, the one named last changes fastest.
The devices are a block of a 4x4x8 slice.
Arguments:
- h0: bfloat16 [64, 512, 3072], P(('data', 'wg'))
- positions: int32 [64, 512], P(('data', 'wg'))
- norm_attn: float32 [1, 3072], replicated
- norm_mlp: float32 [1, 3072], replicated
- w_query: bfloat16 [1, 3072, 24, 128], P(None, 'wg')
- w_key: bfloat16 [1, 3072, 8, 128], P(None, 'wg')
- w_value: bfloat16 [1, 3072, 8, 128], P(None, 'wg')
- w_out: bfloat16 [1, 3072, 3072], P(None, 'wg')
- w_gate: bfloat16 [1, 3072, 8192], P(None, 'wg')
- w_up: bfloat16 [1, 3072, 8192], P(None, 'wg')
- w_down: bfloat16 [1, 8192, 3072], P(None, 'wg')
- norm_final: float32 [3072], replicated
Outputs:
- output: bfloat16 [64, 512, 3072], P(('data', 'wg'))
All inputs are finite; a program needn't handle non-finite values.
Results may differ from the reference program's by a relative error of at most 0.0172752.
Values are sent between devices in bfloat16 or wider.
A program may use at most 768 MiB of HBM per device.

```python
import jax
import jax.numpy as jnp
from jax import lax

N_SEQS = 64
SEQ_LEN = 512
D_MODEL = 3072
N_HEADS = 24
KV_HEADS = 8
HEAD_DIM = 128
FF_DIM = 8192
N_LAYERS = 1
ROPE_BASE = 10000

Q_BLOCK = min(SEQ_LEN, 256)
N_REP = N_HEADS // KV_HEADS
EPS = 1e-5


def normal_weight(rand_key, shape, fan_in, scale_gain):
    raw_draw = jax.random.normal(rand_key, shape, jnp.float32)
    return (raw_draw * (scale_gain * fan_in ** -0.5)).astype(jnp.bfloat16)


def setup_inputs(seed: int = 0, part: int = 0) -> dict:
    base_key = jax.random.key(seed)
    part_key = jax.random.fold_in(base_key, part)
    act_key, step_key, start_key = jax.random.split(part_key, 3)
    shared = jax.random.split(base_key, 10)
    hidden = jax.random.normal(act_key, (N_SEQS, SEQ_LEN, D_MODEL), jnp.float32)
    pos_steps = jax.random.randint(step_key, (N_SEQS, SEQ_LEN), 1, 4)
    pos_starts = jax.random.randint(start_key, (N_SEQS, 1), 0, SEQ_LEN)
    positions = (pos_starts + jnp.cumsum(pos_steps, axis=1) - 1).astype(jnp.int32)
    q_width = N_HEADS * HEAD_DIM
    return {
        'h0': hidden.astype(jnp.bfloat16),
        'positions': positions,
        'norm_attn': 1.0 + 0.25 * jax.random.normal(shared[0], (N_LAYERS, D_MODEL), jnp.float32),
        'norm_mlp': 1.0 + 0.25 * jax.random.normal(shared[1], (N_LAYERS, D_MODEL), jnp.float32),
        'w_query': normal_weight(shared[2], (N_LAYERS, D_MODEL, N_HEADS, HEAD_DIM), D_MODEL, 2.0),
        'w_key': normal_weight(shared[3], (N_LAYERS, D_MODEL, KV_HEADS, HEAD_DIM), D_MODEL, 1.0),
        'w_value': normal_weight(shared[4], (N_LAYERS, D_MODEL, KV_HEADS, HEAD_DIM), D_MODEL, 1.0),
        'w_out': normal_weight(shared[5], (N_LAYERS, q_width, D_MODEL), q_width, 2.0),
        'w_gate': normal_weight(shared[6], (N_LAYERS, D_MODEL, FF_DIM), D_MODEL, 1.0),
        'w_up': normal_weight(shared[7], (N_LAYERS, D_MODEL, FF_DIM), D_MODEL, 1.0),
        'w_down': normal_weight(shared[8], (N_LAYERS, FF_DIM, D_MODEL), FF_DIM, 1.0),
        'norm_final': 1.0 + 0.25 * jax.random.normal(shared[9], (D_MODEL,), jnp.float32),
    }


def rms_norm(values_in, gain_vec):
    as_f32 = values_in.astype(jnp.float32)
    mean_sq = jnp.mean(as_f32 * as_f32, axis=-1, keepdims=True)
    return (as_f32 * lax.rsqrt(mean_sq + EPS) * gain_vec).astype(jnp.bfloat16)


def rope_tables(positions):
    half_dim = HEAD_DIM // 2
    exponents = jnp.arange(half_dim, dtype=jnp.float32) * (2.0 / HEAD_DIM)
    inv_freq = jnp.power(jnp.float32(ROPE_BASE), -exponents)
    angles = positions.astype(jnp.float32)[..., None] * inv_freq
    return jnp.cos(angles)[:, :, None, :], jnp.sin(angles)[:, :, None, :]


def apply_rope(proj, cos_table, sin_table):
    half_dim = HEAD_DIM // 2
    as_f32 = proj.astype(jnp.float32)
    first_half = as_f32[..., :half_dim]
    second_half = as_f32[..., half_dim:]
    rotated = jnp.concatenate([first_half * cos_table - second_half * sin_table, second_half * cos_table + first_half * sin_table], axis=-1)
    return rotated.astype(jnp.bfloat16)


def seq_attention(seq_args):
    query_seq, key_seq, value_seq = seq_args
    n_blocks = SEQ_LEN // Q_BLOCK
    query_blocks = query_seq.reshape(n_blocks, Q_BLOCK, KV_HEADS, N_REP, HEAD_DIM)
    key_f32 = key_seq.astype(jnp.float32)
    value_f32 = value_seq.astype(jnp.float32)
    key_index = jnp.arange(SEQ_LEN)

    def one_block(block_args):
        query_block, block_idx = block_args
        scores = jnp.einsum('qgrd,kgd->grqk', query_block.astype(jnp.float32), key_f32) * HEAD_DIM ** -0.5
        query_index = block_idx * Q_BLOCK + jnp.arange(Q_BLOCK)
        allowed = key_index[None, :] <= query_index[:, None]
        scores = jnp.where(allowed, scores, -1e30)
        attn_probs = jax.nn.softmax(scores, axis=-1).astype(jnp.bfloat16)
        block_out = jnp.einsum('grqk,kgd->qgrd', attn_probs.astype(jnp.float32), value_f32)
        return block_out.astype(jnp.bfloat16)

    attended = lax.map(one_block, (query_blocks, jnp.arange(n_blocks)))
    return attended.reshape(SEQ_LEN, N_HEADS * HEAD_DIM)


def reference(h0, positions, norm_attn, norm_mlp, w_query, w_key, w_value, w_out, w_gate, w_up, w_down, norm_final):
    n_tokens = N_SEQS * SEQ_LEN
    q_width = N_HEADS * HEAD_DIM
    kv_width = KV_HEADS * HEAD_DIM
    cos_table, sin_table = rope_tables(positions)

    def project(normed, weight, width):
        flat = jnp.dot(normed, weight.reshape(D_MODEL, width), preferred_element_type=jnp.float32)
        return flat.astype(jnp.bfloat16)

    def layer_step(residual, layer_params):
        gain_attn, gain_mlp, layer_query, layer_key, layer_value, layer_out, layer_gate, layer_up, layer_down = layer_params
        normed = rms_norm(residual, gain_attn).reshape(n_tokens, D_MODEL)
        query_proj = project(normed, layer_query, q_width).reshape(N_SEQS, SEQ_LEN, N_HEADS, HEAD_DIM)
        key_proj = project(normed, layer_key, kv_width).reshape(N_SEQS, SEQ_LEN, KV_HEADS, HEAD_DIM)
        value_proj = project(normed, layer_value, kv_width).reshape(N_SEQS, SEQ_LEN, KV_HEADS, HEAD_DIM)
        query_proj = apply_rope(query_proj, cos_table, sin_table).reshape(N_SEQS, SEQ_LEN, KV_HEADS, N_REP, HEAD_DIM)
        key_proj = apply_rope(key_proj, cos_table, sin_table)
        attended = lax.map(seq_attention, (query_proj, key_proj, value_proj)).reshape(n_tokens, q_width)
        attn_out = jnp.dot(attended, layer_out, preferred_element_type=jnp.float32)
        residual = (residual.astype(jnp.float32) + attn_out.reshape(N_SEQS, SEQ_LEN, D_MODEL)).astype(jnp.bfloat16)
        normed = rms_norm(residual, gain_mlp).reshape(n_tokens, D_MODEL)
        gate_proj = jnp.dot(normed, layer_gate, preferred_element_type=jnp.float32)
        up_proj = jnp.dot(normed, layer_up, preferred_element_type=jnp.float32)
        hidden = (jax.nn.silu(gate_proj) * up_proj).astype(jnp.bfloat16)
        down_proj = jnp.dot(hidden, layer_down, preferred_element_type=jnp.float32)
        residual = (residual.astype(jnp.float32) + down_proj.reshape(N_SEQS, SEQ_LEN, D_MODEL)).astype(jnp.bfloat16)
        return residual, None

    final_state, unused_out = lax.scan(layer_step, h0, (norm_attn, norm_mlp, w_query, w_key, w_value, w_out, w_gate, w_up, w_down))
    return rms_norm(final_state, norm_final)
```

```python
import functools
import math

import jax
import jax.numpy as jnp
from jax import lax
from jax.experimental import pallas as pl
from jax.experimental.pallas import tpu as pltpu
from jax.sharding import PartitionSpec as P

EPS = 1e-5
ROPE_BASE = 10000.0
COLS_A = 512
COLS_B = 256
HALF_FF = COLS_A // 2
LAG = 5
RING = 4
N_RECV = 18
MESH = pl.DeviceIdType.MESH

R_M0, R_P0, R_2A, R_2B = 0, 1, 2, 3
R_0M, R_MM, R_PM, R_2M, R_0N, R_MN = 4, 5, 6, 7, 8, 9
R_0P, R_MP, R_PP, R_2P, R_P2, R_22 = 10, 11, 12, 13, 14, 15
R_TWIN, R_OWN = 16, 17


def rms_norm(values_in, gain_vec):
    as_f32 = values_in.astype(jnp.float32)
    mean_sq = jnp.mean(as_f32 * as_f32, axis=-1, keepdims=True)
    return (as_f32 * lax.rsqrt(mean_sq + EPS) * gain_vec).astype(jnp.bfloat16)


def rope_tables(positions, head_dim):
    half_dim = head_dim // 2
    exponents = jnp.arange(half_dim, dtype=jnp.float32) * (2.0 / head_dim)
    inv_freq = jnp.power(jnp.float32(ROPE_BASE), -exponents)
    angles = positions.astype(jnp.float32)[..., None] * inv_freq
    cos, sin = jnp.cos(angles), jnp.sin(angles)
    return jnp.concatenate([cos, cos], -1), jnp.concatenate([-sin, sin], -1)


class Place:
    def __init__(self):
        me = lax.axis_index('wg')
        self.core = lax.rem(me, 2)
        chip = me // 2
        col, row = lax.rem(chip, RING), chip // RING
        core = self.core
        self.chip = {}
        for dp in (-1, 0, 1, 2):
            for ds in (-1, 0, 1, 2):
                cc = lax.rem(col + dp * (1 - core) + ds * core + RING, RING)
                rr = lax.rem(row + dp * core + ds * (1 - core) + RING, RING)
                self.chip[dp, ds] = rr * RING + cc
        dev = lambda dp, ds: self.chip[dp, ds] * 2 + core
        self.p_up, self.p_dn = dev(1, 0), dev(-1, 0)
        self.s_up, self.s_dn = dev(0, 1), dev(0, -1)
        self.twin = chip * 2 + 1 - core
        self.me = me


class Gather:
    def __init__(self, place, local, full, recv, send, twin_send):
        self.pl, self.local, self.full = place, local, full
        self.recv, self.send_sem, self.twin_send = recv, send, twin_send
        self.half = local.shape[1] // 2

    def spot(self, blk, rel, part=None):
        ref = self.full.at[blk, self.pl.chip[rel], self.pl.core]
        if part is not None:
            ref = ref.at[pl.ds(part * self.half, self.half)]
        return ref

    def copy(self, blk, src, dst, r, dev):
        return pltpu.make_async_remote_copy(
            src_ref=src, dst_ref=dst, send_sem=self.send_sem.at[blk],
            recv_sem=self.recv.at[blk, r], device_id={'wg': dev}, device_id_type=MESH)

    def put(self, blk, rel, r, dev, part=None):
        ref = self.spot(blk, rel, part)
        self.copy(blk, ref, ref, r, dev).start()

    def got(self, blk, rel, r, part=None):
        ref = self.spot(blk, rel, part)
        self.copy(blk, ref, ref, r, self.pl.me).wait_recv()

    def own_copy(self, blk):
        return pltpu.make_async_copy(self.local.at[blk], self.spot(blk, (0, 0)), self.recv.at[blk, R_OWN])

    def twin_copy(self, blk, core):
        ref = self.full.at[blk, :, core]
        return pltpu.make_async_remote_copy(
            src_ref=ref, dst_ref=ref, send_sem=self.twin_send.at[blk],
            recv_sem=self.recv.at[blk, R_TWIN], device_id={'wg': self.pl.twin}, device_id_type=MESH)

    def stage(self, lag, blk):
        w, got, put = self.pl, self.got, self.put
        if lag == 0:
            src, dst = self.local.at[blk], self.spot(blk, (0, 0))
            self.copy(blk, src, dst, R_M0, w.p_up).start()
            self.copy(blk, src, dst, R_P0, w.p_dn).start()
            self.copy(blk, src, dst, R_0M, w.s_up).start()
            self.copy(blk, src, dst, R_0P, w.s_dn).start()
            self.own_copy(blk).start()
        elif lag == 1:
            got(blk, (-1, 0), R_M0)
            put(blk, (-1, 0), R_2A, w.p_up, 0)
            put(blk, (-1, 0), R_MM, w.s_up)
            put(blk, (-1, 0), R_MP, w.s_dn)
            got(blk, (1, 0), R_P0)
            put(blk, (1, 0), R_2B, w.p_dn, 1)
            put(blk, (1, 0), R_PM, w.s_up)
            put(blk, (1, 0), R_PP, w.s_dn)
            got(blk, (0, -1), R_0M)
            put(blk, (0, -1), R_0N, w.s_up)
        elif lag == 2:
            got(blk, (2, 0), R_2A, 0)
            got(blk, (2, 0), R_2B, 1)
            put(blk, (2, 0), R_2M, w.s_up)
            put(blk, (2, 0), R_2P, w.s_dn)
            got(blk, (-1, -1), R_MM)
            put(blk, (-1, -1), R_MN, w.s_up)
            got(blk, (1, 1), R_PP)
            put(blk, (1, 1), R_P2, w.s_dn)
        elif lag == 3:
            got(blk, (2, 1), R_2P)
            put(blk, (2, 1), R_22, w.s_dn)
        elif lag == 4:
            for rel, r in (((1, -1), R_PM), ((2, -1), R_2M), ((0, 1), R_0P), ((-1, 1), R_MP),
                           ((0, 2), R_0N), ((-1, 2), R_MN), ((1, 2), R_P2), ((2, 2), R_22)):
                got(blk, rel, r)
            self.own_copy(blk).wait()
            self.twin_copy(blk, w.core).start()
        else:
            self.twin_copy(blk, 1 - w.core).wait_recv()

    def drain(self, blk):
        whole = self.full.at[blk, pl.ds(0, RING * RING - 1), 0]
        pltpu.make_async_copy(whole, whole, self.send_sem.at[blk]).wait()
        self.twin_copy(blk, self.pl.core).wait_send()


def layer_kernel(dims, h0, w_a, w_b, cos, sin, gain_attn, gain_mlp, h_out, full_a, full_b,
                 h_s, a_s, heads, u_s, buf_a, buf_b, recv_a, recv_b, send_a, send_b, twin_a, twin_b, load_a, load_b, io_sem):
    n_seq, seq_len, n_heads, kv_heads, head_dim = dims
    n_tok, width = h_s.shape
    n_rep = n_heads // kv_heads
    per_blk = COLS_A // head_dim
    n_a, n_b = w_a.shape[0], w_b.shape[0]
    n_qk, n_v = (n_heads + kv_heads) // per_blk, kv_heads // per_blk
    n_wo = width // COLS_A
    n_gu = u_s.shape[1] // HALF_FF
    first_gu = n_qk + n_v + n_wo
    place = Place()
    ga = Gather(place, w_a, full_a, recv_a, send_a, twin_a)
    gb = Gather(place, w_b, full_b, recv_b, send_b, twin_b)

    barrier = pltpu.get_barrier_semaphore()
    near = (place.p_up, place.p_dn, place.s_up, place.s_dn, place.twin)
    for dev in near:
        pl.semaphore_signal(barrier, inc=1, device_id={'wg': dev}, device_id_type=MESH)
    pl.semaphore_wait(barrier, len(near))

    def tick(t, may_a=True, may_b=True):
        for lag in range(LAG + 1):
            blk = t - lag
            if may_a:
                @pl.when(jnp.logical_and(blk >= 0, blk < n_a))
                def _():
                    ga.stage(lag, blk)
            if may_b:
                @pl.when(jnp.logical_and(blk >= n_a, blk < n_a + n_b))
                def _():
                    gb.stage(lag, blk - n_a)

    def load_copy_a(i):
        slot = lax.rem(i, 2)
        return pltpu.make_async_copy(full_a.at[i], buf_a.at[slot], load_a.at[slot])

    def load_copy_b(i):
        slot = lax.rem(i, 2)
        return pltpu.make_async_copy(full_b.at[i], buf_b.at[slot], load_b.at[slot])

    def weights_a(i):
        return buf_a[lax.rem(i, 2)].reshape(-1, COLS_A)

    def weights_b(i):
        return buf_b[lax.rem(i, 2)].reshape(-1, COLS_B)

    def dot(x, w):
        return jnp.dot(x, w, preferred_element_type=jnp.float32)

    def norm_into(gain):
        rows = min(64, seq_len)

        def body(i, _):
            sl = pl.ds(pl.multiple_of(i * rows, rows), rows)
            a_s[sl, :] = rms_norm(h_s[sl, :], gain[...])
            return 0
        lax.fori_loop(0, n_tok // rows, body, 0)

    def over_seqs(body):
        def step(b, _):
            body(pl.ds(pl.multiple_of(b * seq_len, seq_len), seq_len))
            return 0
        lax.fori_loop(0, n_seq, step, 0)

    def project(i, rope):
        load_copy_a(i).wait()
        load_copy_a(i + 1).start()

        def body(rows):
            out = dot(a_s[rows, :], weights_a(i)).astype(jnp.bfloat16)
            for j in range(per_blk):
                one = out[:, j * head_dim:(j + 1) * head_dim]
                if rope:
                    one = one.astype(jnp.float32)
                    one = (one * cos[rows, :] + pltpu.roll(one, head_dim // 2, 1) * sin[rows, :]).astype(jnp.bfloat16)
                heads[i * per_blk + j, rows, :] = one
        over_seqs(body)

    q_block = seq_len // 2

    def attend(n):
        seq, group = n // kv_heads, lax.rem(n, kv_heads)
        start = pl.multiple_of(seq * seq_len, seq_len)
        for qb in range(2):
            n_keys = (qb + 1) * q_block
            keys = heads[n_heads + group, pl.ds(start, n_keys), :]
            vals = heads[n_heads + kv_heads + group, pl.ds(start, n_keys), :]
            q_rows = pl.ds(pl.multiple_of(start + qb * q_block, q_block), q_block)
            q_idx = qb * q_block + lax.broadcasted_iota(jnp.int32, (q_block, n_keys), 0)
            k_idx = lax.broadcasted_iota(jnp.int32, (q_block, n_keys), 1)
            for r in range(n_rep):
                head = group * n_rep + r
                scores = lax.dot_general(heads[head, q_rows, :], keys, (((1,), (1,)), ((), ())),
                                         preferred_element_type=jnp.float32) * head_dim ** -0.5
                scores = jnp.where(k_idx <= q_idx, scores, -1e30)
                top = jnp.max(scores, axis=-1, keepdims=True)
                expd = jnp.exp(scores - top)
                total = jnp.sum(expd, axis=-1, keepdims=True)
                probs = (expd / total).astype(jnp.bfloat16)
                cols = pl.ds(pl.multiple_of(head * head_dim, head_dim), head_dim)
                a_s[q_rows, cols] = dot(probs, vals).astype(jnp.bfloat16)

    def project_out(i):
        blk = n_qk + n_v + i
        load_copy_a(blk).wait()
        load_copy_a(blk + 1).start()
        cols = pl.ds(pl.multiple_of(i * COLS_A, COLS_A), COLS_A)

        def body(rows):
            out = dot(a_s[rows, :], weights_a(blk))
            h_s[rows, cols] = (h_s[rows, cols].astype(jnp.float32) + out).astype(jnp.bfloat16)
        over_seqs(body)

    def gate_up(i):
        blk = first_gu + i
        load_copy_a(blk).wait()

        @pl.when(i + 1 < n_gu)
        def _():
            load_copy_a(blk + 1).start()

        @pl.when(i + 1 == n_gu)
        def _():
            load_copy_b(0).start()
        cols = pl.ds(pl.multiple_of(i * HALF_FF, HALF_FF), HALF_FF)

        def body(rows):
            out = dot(a_s[rows, :], weights_a(blk))
            gate, up = out[:, :HALF_FF], out[:, HALF_FF:]
            u_s[rows, cols] = (gate * jax.nn.sigmoid(gate) * up).astype(jnp.bfloat16)
        over_seqs(body)

    def down(i):
        load_copy_b(i).wait()

        @pl.when(i + 1 < n_b)
        def _():
            load_copy_b(i + 1).start()
        cols = pl.ds(pl.multiple_of(i * COLS_B, COLS_B), COLS_B)

        def body(rows):
            out = dot(u_s[rows, :], weights_b(i))
            h_s[rows, cols] = (h_s[rows, cols].astype(jnp.float32) + out).astype(jnp.bfloat16)
        over_seqs(body)

    def loop(lo, hi, body):
        def step(i, _):
            body(i)
            return 0
        lax.fori_loop(lo, hi, step, 0)

    h_in = pltpu.make_async_copy(h0, h_s, io_sem.at[0])
    h_in.start()
    tick(0, may_b=False)
    h_in.wait()
    norm_into(gain_attn)
    now = 1
    only_a = functools.partial(tick, may_b=n_a <= 0)
    assert n_a > LAG + 1 + n_qk + n_v + n_seq * kv_heads // 2 + n_wo
    loop(now, LAG + 1, only_a)
    now = LAG + 1
    load_copy_a(0).start()

    def seg_qk(i):
        only_a(i + LAG + 1)
        project(i, True)

    def seg_v(i):
        only_a(i + LAG + 1)
        project(i, False)
    loop(0, n_qk, seg_qk)
    loop(n_qk, n_qk + n_v, seg_v)
    now += n_qk + n_v
    att_from = now

    def seg_att(i):
        only_a(att_from + i)
        attend(2 * i)
        attend(2 * i + 1)
    n_att = n_seq * kv_heads // 2
    loop(0, n_att, seg_att)
    now += n_att
    wo_from = now

    def seg_wo(i):
        only_a(wo_from + i)
        project_out(i)
    loop(0, n_wo, seg_wo)
    now += n_wo
    norm_into(gain_mlp)
    rounds = n_gu // 4
    need = max(first_gu + 4 * i + 4 + LAG - (3 * i + 2) for i in range(rounds))
    if now < need:
        loop(now, need, tick)
        now = need
    gu_from = now

    def seg_gu(i):
        t = gu_from + 3 * i
        tick(t)
        gate_up(4 * i)
        tick(t + 1)
        gate_up(4 * i + 1)
        tick(t + 2)
        gate_up(4 * i + 2)
        gate_up(4 * i + 3)
    loop(0, rounds, seg_gu)
    now += 3 * rounds
    need = n_a + LAG + 1
    if now < need:
        loop(now, need, tick)
        now = need
    down_from = now
    late = functools.partial(tick, may_a=down_from < n_a + LAG)

    def seg_down(i):
        late(down_from + i)
        down(i)
    loop(0, n_b, seg_down)

    out_copy = pltpu.make_async_copy(h_s, h_out, io_sem.at[1])
    out_copy.start()
    loop(0, n_a, ga.drain)
    loop(0, n_b, gb.drain)
    out_copy.wait()


def run_layer(h0, cos, sin, gain_attn, gain_mlp, w_query, w_key, w_value, w_out, w_gate, w_up, w_down, n_dev):
    n_seq, seq_len, width = h0.shape
    rows, n_heads, head_dim = w_query.shape
    kv_heads = w_key.shape[1]
    n_tok = n_seq * seq_len
    ff = w_gate.shape[1]
    rows_b = w_down.shape[0]

    def blocks(weight, cols):
        return weight.reshape(weight.shape[0], -1, cols).transpose(1, 0, 2)

    gu = jnp.concatenate([blocks(w_gate, HALF_FF), blocks(w_up, HALF_FF)], axis=-1)
    w_a = jnp.concatenate([
        blocks(w_query.reshape(rows, -1), COLS_A), blocks(w_key.reshape(rows, -1), COLS_A),
        blocks(w_value.reshape(rows, -1), COLS_A), blocks(w_out, COLS_A), gu], axis=0)
    w_b = blocks(w_down, COLS_B)
    n_a, n_b = w_a.shape[0], w_b.shape[0]
    chips = n_dev // 2
    any_spec = pl.BlockSpec(memory_space=pl.ANY)
    vmem_spec = pl.BlockSpec(memory_space=pltpu.VMEM)
    flops = 2 * n_tok * n_dev * (w_a.size + w_b.size)
    h_out, _, _ = pl.pallas_call(
        functools.partial(layer_kernel, (n_seq, seq_len, n_heads, kv_heads, head_dim)),
        out_shape=(
            jax.ShapeDtypeStruct((n_tok, width), jnp.bfloat16),
            jax.ShapeDtypeStruct((n_a, chips, 2, rows, COLS_A), jnp.bfloat16),
            jax.ShapeDtypeStruct((n_b, chips, 2, rows_b, COLS_B), jnp.bfloat16),
        ),
        in_specs=[any_spec] * 3 + [vmem_spec] * 4,
        out_specs=(any_spec,) * 3,
        scratch_shapes=[
            pltpu.VMEM((n_tok, width), jnp.bfloat16),
            pltpu.VMEM((n_tok, width), jnp.bfloat16),
            pltpu.VMEM((n_heads + 2 * kv_heads, n_tok, head_dim), jnp.bfloat16),
            pltpu.VMEM((n_tok, ff), jnp.bfloat16),
            pltpu.VMEM((2, chips, 2, rows, COLS_A), jnp.bfloat16),
            pltpu.VMEM((2, chips, 2, rows_b, COLS_B), jnp.bfloat16),
            pltpu.SemaphoreType.DMA((n_a, N_RECV)),
            pltpu.SemaphoreType.DMA((n_b, N_RECV)),
            pltpu.SemaphoreType.DMA((n_a,)),
            pltpu.SemaphoreType.DMA((n_b,)),
            pltpu.SemaphoreType.DMA((n_a,)),
            pltpu.SemaphoreType.DMA((n_b,)),
            pltpu.SemaphoreType.DMA((2,)),
            pltpu.SemaphoreType.DMA((2,)),
            pltpu.SemaphoreType.DMA((2,)),
        ],
        compiler_params=pltpu.CompilerParams(
            collective_id=0, has_side_effects=True, vmem_limit_bytes=66_000_000),
        cost_estimate=pl.CostEstimate(flops=flops, bytes_accessed=4 * n_dev * (w_a.size + w_b.size), transcendentals=0),
        name='prefill_layer',
    )(h0.reshape(n_tok, width), w_a, w_b, cos, sin, gain_attn[None], gain_mlp[None])
    return h_out.reshape(n_seq, seq_len, width)


def solution(mesh):
    token_spec = P(('data', 'wg'))
    weight_spec = P(None, 'wg')
    whole_spec = P()
    in_specs = (token_spec, token_spec, whole_spec, whole_spec, weight_spec, weight_spec, weight_spec, weight_spec, weight_spec, weight_spec, weight_spec, whole_spec)
    n_dev = mesh.shape['wg']
    assert n_dev == 2 * RING * RING

    def local_forward(h0, positions, norm_attn, norm_mlp, w_query, w_key, w_value, w_out, w_gate, w_up, w_down, norm_final):
        cos, sin = rope_tables(positions.reshape(-1), w_query.shape[-1])
        residual = h0
        for l in range(w_query.shape[0]):
            residual = run_layer(residual, cos, sin, norm_attn[l], norm_mlp[l], w_query[l], w_key[l], w_value[l],
                                 w_out[l], w_gate[l], w_up[l], w_down[l], n_dev)
        return rms_norm(residual, norm_final)

    return jax.shard_map(local_forward, mesh=mesh, in_specs=in_specs, out_specs=token_spec, check_vma=False)
```

```python
import functools
import math

import jax
import jax.numpy as jnp
from jax import lax
from jax.experimental import pallas as pl
from jax.experimental.pallas import tpu as pltpu
from jax.sharding import PartitionSpec as P

EPS = 1e-5
ROPE_BASE = 10000.0
COLS = 256
LAG = 5
RING = 4
N_RECV = 18
MESH = pl.DeviceIdType.MESH

R_M0, R_P0, R_2A, R_2B = 0, 1, 2, 3
R_0M, R_MM, R_PM, R_2M, R_0N, R_MN = 4, 5, 6, 7, 8, 9
R_0P, R_MP, R_PP, R_2P, R_P2, R_22 = 10, 11, 12, 13, 14, 15
R_TWIN, R_OWN = 16, 17


def rms_norm(values_in, gain_vec):
    as_f32 = values_in.astype(jnp.float32)
    mean_sq = jnp.mean(as_f32 * as_f32, axis=-1, keepdims=True)
    return (as_f32 * lax.rsqrt(mean_sq + EPS) * gain_vec).astype(jnp.bfloat16)


def rope_tables(positions, head_dim):
    half_dim = head_dim // 2
    lane = jnp.arange(head_dim)
    exponents = (lane % half_dim).astype(jnp.float32) * (2.0 / head_dim)
    inv_freq = jnp.power(jnp.float32(ROPE_BASE), -exponents)
    angles = positions.astype(jnp.float32)[..., None] * inv_freq
    return jnp.cos(angles), jnp.where(lane < half_dim, -1.0, 1.0) * jnp.sin(angles)


class Place:
    def __init__(self):
        me = lax.axis_index('wg')
        self.core = lax.rem(me, 2)
        chip = me // 2
        col, row = lax.rem(chip, RING), chip // RING
        core = self.core
        self.chip = {}
        for dp in (-1, 0, 1, 2):
            for ds in (-1, 0, 1, 2):
                cc = lax.rem(col + dp * (1 - core) + ds * core + RING, RING)
                rr = lax.rem(row + dp * core + ds * (1 - core) + RING, RING)
                self.chip[dp, ds] = rr * RING + cc
        dev = lambda dp, ds: self.chip[dp, ds] * 2 + core
        self.p_up, self.p_dn = dev(1, 0), dev(-1, 0)
        self.s_up, self.s_dn = dev(0, 1), dev(0, -1)
        self.twin = chip * 2 + 1 - core
        self.me = me


class Gather:
    def __init__(self, place, own, full, recv, send, twin_send):
        self.pl, self.own, self.full = place, own, full
        self.recv, self.send_sem, self.twin_send = recv, send, twin_send

    def spot(self, blk, rel, part=None):
        ref = self.full.at[blk, self.pl.chip[rel], self.pl.core]
        return ref if part is None else ref.at[part]

    def copy(self, blk, src, dst, r, dev):
        return pltpu.make_async_remote_copy(
            src_ref=src, dst_ref=dst, send_sem=self.send_sem.at[blk],
            recv_sem=self.recv.at[blk, r], device_id={'wg': dev}, device_id_type=MESH)

    def put(self, blk, rel, r, dev, part=None):
        ref = self.spot(blk, rel, part)
        self.copy(blk, ref, ref, r, dev).start()

    def got(self, blk, rel, r, part=None):
        ref = self.spot(blk, rel, part)
        self.copy(blk, ref, ref, r, self.pl.me).wait_recv()

    def first(self, blk, own):
        w = self.pl
        for r, dev in ((R_M0, w.p_up), (R_P0, w.p_dn), (R_0M, w.s_up), (R_0P, w.s_dn)):
            for part in range(2):
                self.copy(blk, own(blk, part), self.spot(blk, (0, 0), part), r, dev).start()
        for part in range(2):
            pltpu.make_async_copy(own(blk, part), self.spot(blk, (0, 0), part), self.recv.at[blk, R_OWN]).start()

    def own_wait(self, blk):
        ref = self.spot(blk, (0, 0))
        pltpu.make_async_copy(ref, ref, self.recv.at[blk, R_OWN]).wait()

    def twin_copy(self, blk, core):
        ref = self.full.at[blk, :, core]
        return pltpu.make_async_remote_copy(
            src_ref=ref, dst_ref=ref, send_sem=self.twin_send.at[blk],
            recv_sem=self.recv.at[blk, R_TWIN], device_id={'wg': self.pl.twin}, device_id_type=MESH)

    def stage(self, lag, blk):
        w, got, put = self.pl, self.got, self.put
        if lag == 0:
            for lo, hi, own in self.own:
                if lo == hi:
                    continue
                if len(self.own) == 1:
                    self.first(blk, own)
                else:
                    @pl.when(jnp.logical_and(blk >= lo, blk < hi))
                    def _():
                        self.first(blk, own)
        elif lag == 1:
            got(blk, (-1, 0), R_M0)
            put(blk, (-1, 0), R_2A, w.p_up, 0)
            put(blk, (-1, 0), R_MM, w.s_up)
            put(blk, (-1, 0), R_MP, w.s_dn)
            got(blk, (1, 0), R_P0)
            put(blk, (1, 0), R_2B, w.p_dn, 1)
            put(blk, (1, 0), R_PM, w.s_up)
            put(blk, (1, 0), R_PP, w.s_dn)
            got(blk, (0, -1), R_0M)
            put(blk, (0, -1), R_0N, w.s_up)
        elif lag == 2:
            got(blk, (2, 0), R_2A, 0)
            got(blk, (2, 0), R_2B, 1)
            put(blk, (2, 0), R_2M, w.s_up)
            put(blk, (2, 0), R_2P, w.s_dn)
            got(blk, (-1, -1), R_MM)
            put(blk, (-1, -1), R_MN, w.s_up)
            got(blk, (1, 1), R_PP)
            put(blk, (1, 1), R_P2, w.s_dn)
        elif lag == 3:
            got(blk, (2, 1), R_2P)
            put(blk, (2, 1), R_22, w.s_dn)
        elif lag == 4:
            for rel, r in (((1, -1), R_PM), ((2, -1), R_2M), ((0, 1), R_0P), ((-1, 1), R_MP),
                           ((0, 2), R_0N), ((-1, 2), R_MN), ((1, 2), R_P2), ((2, 2), R_22)):
                got(blk, rel, r)
            self.own_wait(blk)
            self.twin_copy(blk, w.core).start()
        else:
            self.twin_copy(blk, 1 - w.core).wait_recv()

    def drain(self, blk):
        whole = self.full.at[blk, pl.ds(0, RING * RING - 1), 0]
        pltpu.make_async_copy(whole, whole, self.send_sem.at[blk]).wait()
        self.twin_copy(blk, self.pl.core).wait_send()


def layer_kernel(dims, h0, w_q, w_k, w_v, w_o, w_g, w_u, w_d, cos, sin, gain_attn, gain_mlp, gain_out, out_ref, full_a, full_b,
                 h_s, a_s, heads, u_s, acc_s, buf_a, buf_b, recv_a, recv_b, send_a, send_b, twin_a, twin_b, load_a, load_b, io_sem):
    n_seq, seq_len, n_heads, kv_heads, head_dim = dims
    n_tok, width = h_s.shape
    n_rep = n_heads // kv_heads
    blk_cols = 2 * COLS
    per_part = COLS // head_dim
    n_q, n_k = n_heads * head_dim // blk_cols, kv_heads * head_dim // blk_cols
    n_qk, n_v = n_q + n_k, n_k
    n_wo = width // blk_cols
    n_gu = w_g.shape[1] // COLS
    first_gu = n_qk + n_v + n_wo
    n_a = first_gu + n_gu
    rows_b = w_d.shape[0]
    half_b = rows_b // 2
    n_b = 2 * (width // COLS)
    place = Place()

    def cols_of(ref, blk, part):
        return ref.at[:, pl.ds(pl.multiple_of((2 * blk + part) * COLS, COLS), COLS)]

    def ff_cols(blk, part):
        return (w_g, w_u)[part].at[:, pl.ds(pl.multiple_of((blk - first_gu) * COLS, COLS), COLS)]

    def down_part(blk, part):
        quarter = half_b // 2
        return w_d.at[pl.ds(pl.multiple_of(lax.rem(blk, 2) * half_b + part * quarter, quarter), quarter),
                      pl.ds(pl.multiple_of(blk // 2 * COLS, COLS), COLS)]
    own_a = [(0, n_q, lambda blk, part: cols_of(w_q, blk, part)),
             (n_q, n_qk, lambda blk, part: cols_of(w_k, blk - n_q, part)),
             (n_qk, n_qk + n_v, lambda blk, part: cols_of(w_v, blk - n_qk, part)),
             (n_qk + n_v, first_gu, lambda blk, part: cols_of(w_o, blk - n_qk - n_v, part)),
             (first_gu, n_a, ff_cols)]
    ga = Gather(place, own_a, full_a, recv_a, send_a, twin_a)
    gb = Gather(place, [(0, n_b, down_part)], full_b, recv_b, send_b, twin_b)

    barrier = pltpu.get_barrier_semaphore()
    near = (place.p_up, place.p_dn, place.s_up, place.s_dn, place.twin)
    for dev in near:
        pl.semaphore_signal(barrier, inc=1, device_id={'wg': dev}, device_id_type=MESH)
    pl.semaphore_wait(barrier, len(near))

    def tick(t, may_a=True, may_b=True):
        for lag in range(LAG + 1):
            blk = t - lag
            if may_a:
                @pl.when(jnp.logical_and(blk >= 0, blk < n_a))
                def _():
                    ga.stage(lag, blk)
            if may_b:
                @pl.when(jnp.logical_and(blk >= n_a, blk < n_a + n_b))
                def _():
                    gb.stage(lag, blk - n_a)

    def load_copy_a(i):
        slot = lax.rem(i, 2)
        return pltpu.make_async_copy(full_a.at[i], buf_a.at[slot], load_a.at[slot])

    def load_copy_b(i):
        slot = lax.rem(i, 2)
        return pltpu.make_async_copy(full_b.at[i], buf_b.at[slot], load_b.at[slot])

    def weights_a(i, part):
        return buf_a[lax.rem(i, 2), :, :, part].reshape(width, COLS)

    def weights_b(i):
        return buf_b[lax.rem(i, 2)].reshape(-1, COLS)

    def dot(x, w):
        return jnp.dot(x, w, preferred_element_type=jnp.float32)

    norm_rows = min(64, seq_len)

    def norm_into(gain, lo, hi):
        def body(i, _):
            sl = pl.ds(pl.multiple_of(i * norm_rows, norm_rows), norm_rows)
            a_s[sl, :] = rms_norm(h_s[sl, :], gain[...])
            return 0
        lax.fori_loop(lo, hi, body, 0)

    def over_seqs(body):
        def step(b, _):
            body(pl.ds(pl.multiple_of(b * seq_len, seq_len), seq_len))
            return 0
        lax.fori_loop(0, n_seq, step, 0)

    def project(i, rope):
        load_copy_a(i).wait()
        load_copy_a(i + 1).start()

        def body(rows):
            for part in range(2):
                out = dot(a_s[rows, :], weights_a(i, part)).astype(jnp.bfloat16)
                for j in range(per_part):
                    one = out[:, j * head_dim:(j + 1) * head_dim]
                    if rope:
                        one = one.astype(jnp.float32)
                        one = (one * cos[rows, :] + pltpu.roll(one, head_dim // 2, 1) * sin[rows, :]).astype(jnp.bfloat16)
                    heads[(2 * i + part) * per_part + j, rows, :] = one
        over_seqs(body)

    q_block = seq_len // 2

    def attend(n):
        seq, group = n // kv_heads, lax.rem(n, kv_heads)
        start = pl.multiple_of(seq * seq_len, seq_len)
        for qb in range(2):
            n_keys = (qb + 1) * q_block
            keys = heads[n_heads + group, pl.ds(start, n_keys), :]
            vals = heads[n_heads + kv_heads + group, pl.ds(start, n_keys), :]
            q_rows = pl.ds(pl.multiple_of(start + qb * q_block, q_block), q_block)
            q_idx = qb * q_block + lax.broadcasted_iota(jnp.int32, (q_block, n_keys), 0)
            k_idx = lax.broadcasted_iota(jnp.int32, (q_block, n_keys), 1)
            for r in range(n_rep):
                head = group * n_rep + r
                scores = lax.dot_general(heads[head, q_rows, :], keys, (((1,), (1,)), ((), ())),
                                         preferred_element_type=jnp.float32) * head_dim ** -0.5
                scores = jnp.where(k_idx <= q_idx, scores, -1e30)
                top = jnp.max(scores, axis=-1, keepdims=True)
                expd = jnp.exp(scores - top)
                total = jnp.sum(expd, axis=-1, keepdims=True)
                probs = (expd / total).astype(jnp.bfloat16)
                cols = pl.ds(pl.multiple_of(head * head_dim, head_dim), head_dim)
                a_s[q_rows, cols] = dot(probs, vals).astype(jnp.bfloat16)

    def project_out(i):
        blk = n_qk + n_v + i
        load_copy_a(blk).wait()
        load_copy_a(blk + 1).start()

        def body(rows):
            for part in range(2):
                cols = pl.ds(pl.multiple_of((2 * i + part) * COLS, COLS), COLS)
                out = dot(a_s[rows, :], weights_a(blk, part))
                h_s[rows, cols] = (h_s[rows, cols].astype(jnp.float32) + out).astype(jnp.bfloat16)
        over_seqs(body)

    def gate_up(i):
        blk = first_gu + i
        load_copy_a(blk).wait()

        @pl.when(i + 1 < n_gu)
        def _():
            load_copy_a(blk + 1).start()

        @pl.when(i + 1 == n_gu)
        def _():
            load_copy_b(0).start()
        n_own = COLS // rows_b

        def body(rows):
            gate = dot(a_s[rows, :], weights_a(blk, 0))
            up = dot(a_s[rows, :], weights_a(blk, 1))
            u = (gate * jax.nn.sigmoid(gate) * up).astype(jnp.bfloat16)
            for j in range(n_own):
                to = pl.ds(pl.multiple_of((i * n_own + j) * half_b, half_b), half_b)
                for half in range(2):
                    u_s[half, rows, to] = u[:, j * rows_b + half * half_b:j * rows_b + (half + 1) * half_b]
        over_seqs(body)

    def down(i):
        load_copy_b(i).wait()

        @pl.when(i + 1 < n_b)
        def _():
            load_copy_b(i + 1).start()
        cols = pl.ds(pl.multiple_of(i // 2 * COLS, COLS), COLS)

        def first_half(rows):
            acc_s[rows, :] = dot(u_s[0, rows, :], weights_b(i))

        def second_half(rows):
            out = acc_s[rows, :] + dot(u_s[1, rows, :], weights_b(i))
            h_s[rows, cols] = (h_s[rows, cols].astype(jnp.float32) + out).astype(jnp.bfloat16)

        @pl.when(lax.rem(i, 2) == 0)
        def _():
            over_seqs(first_half)

        @pl.when(lax.rem(i, 2) == 1)
        def _():
            over_seqs(second_half)

    def loop(lo, hi, body):
        def step(i, _):
            body(i)
            return 0
        lax.fori_loop(lo, hi, step, 0)

    h_in = pltpu.make_async_copy(h0, h_s, io_sem.at[0])
    h_in.start()
    only_a = functools.partial(tick, may_b=False)
    n_norm = n_tok // norm_rows
    only_a(0)
    only_a(1)
    h_in.wait()
    now = 2
    share = -(-n_norm // (LAG + 1 - now))

    def seg_start(i):
        only_a(i)
        norm_into(gain_attn, (i - 2) * share, jnp.minimum((i - 1) * share, n_norm))
    assert n_a > LAG + 1 + n_qk + n_v + n_seq * kv_heads // 2 + n_wo
    loop(now, LAG + 1, seg_start)
    now = LAG + 1
    load_copy_a(0).start()

    def seg_qk(i):
        only_a(i + LAG + 1)
        project(i, True)

    def seg_v(i):
        only_a(i + LAG + 1)
        project(i, False)
    loop(0, n_qk, seg_qk)
    loop(n_qk, n_qk + n_v, seg_v)
    now += n_qk + n_v
    att_from = now

    def seg_att(i):
        only_a(att_from + i)
        attend(2 * i)
        attend(2 * i + 1)
    n_att = n_seq * kv_heads // 2
    loop(0, n_att, seg_att)
    now += n_att
    wo_from = now

    def seg_wo(i):
        only_a(wo_from + i)
        project_out(i)
    loop(0, n_wo, seg_wo)
    now += n_wo
    norm_into(gain_mlp, 0, n_norm)
    rounds = n_gu // 4
    need = max(first_gu + 4 * i + 4 + LAG - (3 * i + 2) for i in range(rounds))
    if now < need:
        loop(now, need, tick)
        now = need
    gu_from = now

    def seg_gu(i):
        t = gu_from + 3 * i
        tick(t)
        gate_up(4 * i)
        tick(t + 1)
        gate_up(4 * i + 1)
        tick(t + 2)
        gate_up(4 * i + 2)
        gate_up(4 * i + 3)
    loop(0, rounds, seg_gu)
    now += 3 * rounds
    need = n_a + LAG + 1
    if now < need:
        loop(now, need, tick)
        now = need
    down_from = now
    late = functools.partial(tick, may_a=down_from < n_a + LAG)

    def seg_down(i):
        late(down_from + i)
        down(i)
    loop(0, n_b, seg_down)

    if gain_out is None:
        out_copy = pltpu.make_async_copy(h_s, out_ref, io_sem.at[1])
        out_copy.start()
    else:
        def finish(i):
            sl = pl.ds(pl.multiple_of(i * norm_rows, norm_rows), norm_rows)
            a_s[sl, :] = rms_norm(h_s[sl, :], gain_out[...])

            @pl.when(i > 0)
            def _():
                put_out(i - 1)

        def put_out(i):
            sl = pl.ds(pl.multiple_of(i * norm_rows, norm_rows), norm_rows)
            pltpu.make_async_copy(a_s.at[sl], out_ref.at[sl], io_sem.at[1]).start()
        loop(0, n_norm, finish)
        out_copy = pltpu.make_async_copy(a_s, out_ref, io_sem.at[1])
    loop(0, n_a, ga.drain)
    loop(0, n_b, gb.drain)
    if gain_out is not None:
        put_out(n_norm - 1)
    out_copy.wait()


def run_layer(h0, cos, sin, gain_attn, gain_mlp, gain_out, w_query, w_key, w_value, w_out, w_gate, w_up, w_down, n_dev):
    n_seq, seq_len, width = h0.shape
    rows, n_heads, head_dim = w_query.shape
    kv_heads = w_key.shape[1]
    n_tok = n_seq * seq_len
    ff = w_gate.shape[1]
    rows_b = w_down.shape[0]
    w_q, w_k, w_v = (w.reshape(rows, -1) for w in (w_query, w_key, w_value))
    n_a = (w_q.shape[1] + w_k.shape[1] + w_v.shape[1] + width) // (2 * COLS) + ff // COLS
    n_b = 2 * (width // COLS)
    chips = n_dev // 2
    any_spec = pl.BlockSpec(memory_space=pl.ANY)
    vmem_spec = pl.BlockSpec(memory_space=pltpu.VMEM)
    n_weights = n_dev * (n_a * rows * 2 * COLS + rows_b * width)
    last = gain_out is not None
    body = functools.partial(layer_kernel, (n_seq, seq_len, n_heads, kv_heads, head_dim))
    operands = [h0.reshape(n_tok, width), w_q, w_k, w_v, w_out, w_gate, w_up, w_down, cos, sin, gain_attn[None], gain_mlp[None]]
    if last:
        operands.append(gain_out[None])
        kernel = body
    else:
        def kernel(*refs):
            return body(*refs[:12], None, *refs[12:])
    out, _, _ = pl.pallas_call(
        kernel,
        out_shape=(
            jax.ShapeDtypeStruct((n_tok, width), jnp.bfloat16),
            jax.ShapeDtypeStruct((n_a, chips, 2, 2, rows, COLS), jnp.bfloat16),
            jax.ShapeDtypeStruct((n_b, chips, 2, 2, rows_b // 4, COLS), jnp.bfloat16),
        ),
        in_specs=[any_spec] * 8 + [vmem_spec] * (len(operands) - 8),
        out_specs=(any_spec,) * 3,
        scratch_shapes=[
            pltpu.VMEM((n_tok, width), jnp.bfloat16),
            pltpu.VMEM((n_tok, width), jnp.bfloat16),
            pltpu.VMEM((n_heads + 2 * kv_heads, n_tok, head_dim), jnp.bfloat16),
            pltpu.VMEM((2, n_tok, ff // 2), jnp.bfloat16),
            pltpu.VMEM((n_tok, COLS), jnp.float32),
            pltpu.VMEM((2, chips, 2, 2, rows, COLS), jnp.bfloat16),
            pltpu.VMEM((2, chips, 2, 2, rows_b // 4, COLS), jnp.bfloat16),
            pltpu.SemaphoreType.DMA((n_a, N_RECV)),
            pltpu.SemaphoreType.DMA((n_b, N_RECV)),
            pltpu.SemaphoreType.DMA((n_a,)),
            pltpu.SemaphoreType.DMA((n_b,)),
            pltpu.SemaphoreType.DMA((n_a,)),
            pltpu.SemaphoreType.DMA((n_b,)),
            pltpu.SemaphoreType.DMA((2,)),
            pltpu.SemaphoreType.DMA((2,)),
            pltpu.SemaphoreType.DMA((2,)),
        ],
        compiler_params=pltpu.CompilerParams(
            collective_id=0, has_side_effects=True, vmem_limit_bytes=66_000_000),
        cost_estimate=pl.CostEstimate(flops=2 * n_tok * n_weights, bytes_accessed=4 * n_weights, transcendentals=0),
        name='prefill_layer',
    )(*operands)
    return out.reshape(n_seq, seq_len, width)


def solution(mesh):
    token_spec = P(('data', 'wg'))
    weight_spec = P(None, 'wg')
    whole_spec = P()
    in_specs = (token_spec, token_spec, whole_spec, whole_spec, weight_spec, weight_spec, weight_spec, weight_spec, weight_spec, weight_spec, weight_spec, whole_spec)
    n_dev = mesh.shape['wg']
    assert n_dev == 2 * RING * RING

    def local_forward(h0, positions, norm_attn, norm_mlp, w_query, w_key, w_value, w_out, w_gate, w_up, w_down, norm_final):
        cos, sin = rope_tables(positions.reshape(-1), w_query.shape[-1])
        residual = h0
        n_layers = w_query.shape[0]
        for l in range(n_layers):
            residual = run_layer(residual, cos, sin, norm_attn[l], norm_mlp[l], norm_final if l == n_layers - 1 else None,
                                 w_query[l], w_key[l], w_value[l], w_out[l], w_gate[l], w_up[l], w_down[l], n_dev)
        return residual

    return jax.shard_map(local_forward, mesh=mesh, in_specs=in_specs, out_specs=token_spec, check_vma=False)
```

```python
import functools
import math

import jax
import jax.numpy as jnp
from jax import lax
from jax.experimental import pallas as pl
from jax.experimental.pallas import tpu as pltpu
from jax.sharding import PartitionSpec as P

EPS = 1e-5
ROPE_BASE = 10000.0
COLS = 256
LAGS_A = (0, 2, 4, 6, 8, 9)
LAGS_B = (0, 1, 2, 3, 4, 5)
LAG_A, LAG_B = LAGS_A[-1], LAGS_B[-1]
RING = 4
N_RECV = 18
MESH = pl.DeviceIdType.MESH

R_M0, R_P0, R_2A, R_2B = 0, 1, 2, 3
R_0M, R_MM, R_PM, R_2M, R_0N, R_MN = 4, 5, 6, 7, 8, 9
R_0P, R_MP, R_PP, R_2P, R_P2, R_22 = 10, 11, 12, 13, 14, 15
R_TWIN, R_OWN = 16, 17


def rms_norm(values_in, gain_vec):
    as_f32 = values_in.astype(jnp.float32)
    mean_sq = jnp.mean(as_f32 * as_f32, axis=-1, keepdims=True)
    return (as_f32 * lax.rsqrt(mean_sq + EPS) * gain_vec).astype(jnp.bfloat16)


def rope_tables(positions, head_dim):
    half_dim = head_dim // 2
    lane = jnp.arange(head_dim)
    exponents = (lane % half_dim).astype(jnp.float32) * (2.0 / head_dim)
    inv_freq = jnp.power(jnp.float32(ROPE_BASE), -exponents)
    angles = positions.astype(jnp.float32)[..., None] * inv_freq
    return jnp.cos(angles), jnp.where(lane < half_dim, -1.0, 1.0) * jnp.sin(angles)


class Place:
    def __init__(self):
        me = lax.axis_index('wg')
        self.core = lax.rem(me, 2)
        chip = me // 2
        col, row = lax.rem(chip, RING), chip // RING
        at = lambda dc, dr: lax.rem(row + dr + RING, RING) * RING + lax.rem(col + dc + RING, RING)
        self.at = {(i, j): at(i, j) for i in (-1, 0, 1, 2) for j in (-1, 0, 1, 2)}
        self.near = tuple(self.at[rel] * 2 + self.core for rel in ((1, 0), (-1, 0), (0, 1), (0, -1)))
        self.twin = chip * 2 + 1 - self.core
        self.me = me

    def chip(self, blk, rel):
        straight, turned = self.at[rel], self.at[rel[::-1]]
        return straight + lax.rem(blk + self.core, 2) * (turned - straight)

    def dev(self, blk, dp, ds):
        return self.chip(blk, (dp, ds)) * 2 + self.core


class Gather:
    def __init__(self, place, own, full, recv, send, twin_send):
        self.pl, self.own, self.full = place, own, full
        self.recv, self.send_sem, self.twin_send = recv, send, twin_send

    def spot(self, blk, rel, part=None):
        ref = self.full.at[blk, self.pl.chip(blk, rel), self.pl.core]
        return ref if part is None else ref.at[part]

    def copy(self, blk, src, dst, r, dev):
        return pltpu.make_async_remote_copy(
            src_ref=src, dst_ref=dst, send_sem=self.send_sem.at[blk],
            recv_sem=self.recv.at[blk, r], device_id={'wg': dev}, device_id_type=MESH)

    def put(self, blk, rel, r, dev, part=None):
        ref = self.spot(blk, rel, part)
        self.copy(blk, ref, ref, r, dev).start()

    def got(self, blk, rel, r, part=None):
        ref = self.spot(blk, rel, part)
        self.copy(blk, ref, ref, r, self.pl.me).wait_recv()

    def first(self, blk, own):
        w = self.pl
        for r, rel in ((R_M0, (1, 0)), (R_P0, (-1, 0)), (R_0M, (0, 1)), (R_0P, (0, -1))):
            dev = w.dev(blk, *rel)
            for part in range(2):
                self.copy(blk, own(blk, part), self.spot(blk, (0, 0), part), r, dev).start()
        for part in range(2):
            pltpu.make_async_copy(own(blk, part), self.spot(blk, (0, 0), part), self.recv.at[blk, R_OWN]).start()

    def own_wait(self, blk):
        ref = self.spot(blk, (0, 0))
        pltpu.make_async_copy(ref, ref, self.recv.at[blk, R_OWN]).wait()

    def twin_copy(self, blk, core):
        ref = self.full.at[blk, :, core]
        return pltpu.make_async_remote_copy(
            src_ref=ref, dst_ref=ref, send_sem=self.twin_send.at[blk],
            recv_sem=self.recv.at[blk, R_TWIN], device_id={'wg': self.pl.twin}, device_id_type=MESH)

    def stage(self, step, blk):
        w, got, put = self.pl, self.got, self.put
        p_up, p_dn, s_up, s_dn = (w.dev(blk, *rel) for rel in ((1, 0), (-1, 0), (0, 1), (0, -1)))
        if step == 0:
            for lo, hi, own in self.own:
                if lo == hi:
                    continue
                if len(self.own) == 1:
                    self.first(blk, own)
                else:
                    @pl.when(jnp.logical_and(blk >= lo, blk < hi))
                    def _():
                        self.first(blk, own)
        elif step == 1:
            got(blk, (-1, 0), R_M0)
            put(blk, (-1, 0), R_2A, p_up, 0)
            put(blk, (-1, 0), R_MM, s_up)
            put(blk, (-1, 0), R_MP, s_dn)
            got(blk, (1, 0), R_P0)
            put(blk, (1, 0), R_2B, p_dn, 1)
            put(blk, (1, 0), R_PM, s_up)
            put(blk, (1, 0), R_PP, s_dn)
            got(blk, (0, -1), R_0M)
            put(blk, (0, -1), R_0N, s_up)
        elif step == 2:
            got(blk, (2, 0), R_2A, 0)
            got(blk, (2, 0), R_2B, 1)
            put(blk, (2, 0), R_2M, s_up)
            put(blk, (2, 0), R_2P, s_dn)
            got(blk, (-1, -1), R_MM)
            put(blk, (-1, -1), R_MN, s_up)
            got(blk, (1, 1), R_PP)
            put(blk, (1, 1), R_P2, s_dn)
        elif step == 3:
            got(blk, (2, 1), R_2P)
            put(blk, (2, 1), R_22, s_dn)
        elif step == 4:
            for rel, r in (((1, -1), R_PM), ((2, -1), R_2M), ((0, 1), R_0P), ((-1, 1), R_MP),
                           ((0, 2), R_0N), ((-1, 2), R_MN), ((1, 2), R_P2), ((2, 2), R_22)):
                got(blk, rel, r)
            self.own_wait(blk)
            self.twin_copy(blk, w.core).start()
        else:
            self.twin_copy(blk, 1 - w.core).wait_recv()

    def drain(self, blk):
        whole = self.full.at[blk, pl.ds(0, RING * RING - 1), 0]
        pltpu.make_async_copy(whole, whole, self.send_sem.at[blk]).wait()
        self.twin_copy(blk, self.pl.core).wait_send()


def layer_kernel(dims, h0, w_q, w_k, w_v, w_o, w_g, w_u, w_d, cos, sin, gain_attn, gain_mlp, out_ref, full_a, full_b,
                 h_s, a_s, heads, u_s, acc_s, buf_a, buf_b, recv_a, recv_b, send_a, send_b, twin_a, twin_b, load_a, load_b, io_sem):
    n_seq, seq_len, n_heads, kv_heads, head_dim = dims
    n_tok, width = h_s.shape
    n_rep = n_heads // kv_heads
    blk_cols = 2 * COLS
    per_part = COLS // head_dim
    n_q, n_k = n_heads * head_dim // blk_cols, kv_heads * head_dim // blk_cols
    n_qk, n_v = n_q + n_k, n_k
    n_wo = width // blk_cols
    n_gu = w_g.shape[1] // COLS
    first_gu = n_qk + n_v + n_wo
    n_a = first_gu + n_gu
    rows_b = w_d.shape[0]
    half_b = rows_b // 2
    n_b = 2 * (width // COLS)
    place = Place()

    def cols_of(ref, blk, part):
        return ref.at[:, pl.ds(pl.multiple_of((2 * blk + part) * COLS, COLS), COLS)]

    def ff_cols(blk, part):
        return (w_g, w_u)[part].at[:, pl.ds(pl.multiple_of((blk - first_gu) * COLS, COLS), COLS)]

    def down_part(blk, part):
        quarter = half_b // 2
        return w_d.at[pl.ds(pl.multiple_of(lax.rem(blk, 2) * half_b + part * quarter, quarter), quarter),
                      pl.ds(pl.multiple_of(blk // 2 * COLS, COLS), COLS)]
    own_a = [(0, n_q, lambda blk, part: cols_of(w_q, blk, part)),
             (n_q, n_qk, lambda blk, part: cols_of(w_k, blk - n_q, part)),
             (n_qk, n_qk + n_v, lambda blk, part: cols_of(w_v, blk - n_qk, part)),
             (n_qk + n_v, first_gu, lambda blk, part: cols_of(w_o, blk - n_qk - n_v, part)),
             (first_gu, n_a, ff_cols)]
    ga = Gather(place, own_a, full_a, recv_a, send_a, twin_a)
    gb = Gather(place, [(0, n_b, down_part)], full_b, recv_b, send_b, twin_b)

    barrier = pltpu.get_barrier_semaphore()
    near = place.near + (place.twin,)
    for dev in near:
        pl.semaphore_signal(barrier, inc=1, device_id={'wg': dev}, device_id_type=MESH)
    pl.semaphore_wait(barrier, len(near))

    def tick(t, may_a=True, may_b=True):
        for step, (lag_a, lag_b) in enumerate(zip(LAGS_A, LAGS_B)):
            if may_a:
                @pl.when(jnp.logical_and(t - lag_a >= 0, t - lag_a < n_a))
                def _():
                    ga.stage(step, t - lag_a)
            if may_b:
                @pl.when(jnp.logical_and(t - lag_b >= n_a, t - lag_b < n_a + n_b))
                def _():
                    gb.stage(step, t - lag_b - n_a)

    def load_copy_a(i):
        slot = lax.rem(i, 2)
        return pltpu.make_async_copy(full_a.at[i], buf_a.at[slot], load_a.at[slot])

    def load_copy_b(i):
        slot = lax.rem(i, 2)
        return pltpu.make_async_copy(full_b.at[i], buf_b.at[slot], load_b.at[slot])

    def weights_a(i, part):
        return buf_a[lax.rem(i, 2), :, :, part].reshape(width, COLS)

    def weights_b(i):
        return buf_b[lax.rem(i, 2)].reshape(-1, COLS)

    def dot(x, w):
        return jnp.dot(x, w, preferred_element_type=jnp.float32)

    norm_rows = min(64, seq_len)

    def norm_into(gain, lo, hi):
        def body(i, _):
            sl = pl.ds(pl.multiple_of(i * norm_rows, norm_rows), norm_rows)
            a_s[sl, :] = rms_norm(h_s[sl, :], gain[...])
            return 0
        lax.fori_loop(lo, hi, body, 0)

    def over_seqs(body):
        def step(b, _):
            body(pl.ds(pl.multiple_of(b * seq_len, seq_len), seq_len))
            return 0
        lax.fori_loop(0, n_seq, step, 0)

    def project(i, rope):
        load_copy_a(i).wait()
        load_copy_a(i + 1).start()

        def body(rows):
            for part in range(2):
                out = dot(a_s[rows, :], weights_a(i, part)).astype(jnp.bfloat16)
                for j in range(per_part):
                    one = out[:, j * head_dim:(j + 1) * head_dim]
                    if rope:
                        one = one.astype(jnp.float32)
                        one = (one * cos[rows, :] + pltpu.roll(one, head_dim // 2, 1) * sin[rows, :]).astype(jnp.bfloat16)
                    heads[(2 * i + part) * per_part + j, rows, :] = one
        over_seqs(body)

    q_block = seq_len // 2

    def attend(n):
        seq, group = n // kv_heads, lax.rem(n, kv_heads)
        start = pl.multiple_of(seq * seq_len, seq_len)
        for qb in range(2):
            n_keys = (qb + 1) * q_block
            keys = heads[n_heads + group, pl.ds(start, n_keys), :]
            vals = heads[n_heads + kv_heads + group, pl.ds(start, n_keys), :]
            q_rows = pl.ds(pl.multiple_of(start + qb * q_block, q_block), q_block)
            q_idx = qb * q_block + lax.broadcasted_iota(jnp.int32, (q_block, n_keys), 0)
            k_idx = lax.broadcasted_iota(jnp.int32, (q_block, n_keys), 1)
            for r in range(n_rep):
                head = group * n_rep + r
                scores = lax.dot_general(heads[head, q_rows, :], keys, (((1,), (1,)), ((), ())),
                                         preferred_element_type=jnp.float32) * head_dim ** -0.5
                scores = jnp.where(k_idx <= q_idx, scores, -1e30)
                top = jnp.max(scores, axis=-1, keepdims=True)
                expd = jnp.exp(scores - top)
                total = jnp.sum(expd, axis=-1, keepdims=True)
                probs = (expd / total).astype(jnp.bfloat16)
                cols = pl.ds(pl.multiple_of(head * head_dim, head_dim), head_dim)
                a_s[q_rows, cols] = dot(probs, vals).astype(jnp.bfloat16)

    def project_out(i):
        blk = n_qk + n_v + i
        load_copy_a(blk).wait()
        load_copy_a(blk + 1).start()

        def body(rows):
            for part in range(2):
                cols = pl.ds(pl.multiple_of((2 * i + part) * COLS, COLS), COLS)
                out = dot(a_s[rows, :], weights_a(blk, part))
                h_s[rows, cols] = (h_s[rows, cols].astype(jnp.float32) + out).astype(jnp.bfloat16)
        over_seqs(body)

    def gate_up(i):
        blk = first_gu + i
        load_copy_a(blk).wait()

        @pl.when(i + 1 < n_gu)
        def _():
            load_copy_a(blk + 1).start()

        @pl.when(i + 1 == n_gu)
        def _():
            load_copy_b(0).start()
        n_own = COLS // rows_b

        def body(rows):
            gate = dot(a_s[rows, :], weights_a(blk, 0))
            up = dot(a_s[rows, :], weights_a(blk, 1))
            u = (gate * jax.nn.sigmoid(gate) * up).astype(jnp.bfloat16)
            for j in range(n_own):
                to = pl.ds(pl.multiple_of((i * n_own + j) * half_b, half_b), half_b)
                for half in range(2):
                    u_s[half, rows, to] = u[:, j * rows_b + half * half_b:j * rows_b + (half + 1) * half_b]
        over_seqs(body)

    def down(i):
        load_copy_b(i).wait()

        @pl.when(i + 1 < n_b)
        def _():
            load_copy_b(i + 1).start()
        cols = pl.ds(pl.multiple_of(i // 2 * COLS, COLS), COLS)

        def first_half(rows):
            acc_s[rows, :] = dot(u_s[0, rows, :], weights_b(i))

        def second_half(rows):
            out = acc_s[rows, :] + dot(u_s[1, rows, :], weights_b(i))
            h_s[rows, cols] = (h_s[rows, cols].astype(jnp.float32) + out).astype(jnp.bfloat16)

        @pl.when(lax.rem(i, 2) == 0)
        def _():
            over_seqs(first_half)

            @pl.when(i > 0)
            def _():
                put_out(i // 2 - 1)

        @pl.when(lax.rem(i, 2) == 1)
        def _():
            over_seqs(second_half)

    def put_out(j):
        cols = pl.ds(pl.multiple_of(j * COLS, COLS), COLS)
        pltpu.make_async_copy(h_s.at[:, cols], out_ref.at[:, cols], io_sem.at[1]).start()

    def loop(lo, hi, body):
        def step(i, _):
            body(i)
            return 0
        lax.fori_loop(lo, hi, step, 0)

    h_in = pltpu.make_async_copy(h0, h_s, io_sem.at[0])
    h_in.start()
    only_a = functools.partial(tick, may_b=False)
    n_norm = n_tok // norm_rows
    only_a(0)
    only_a(1)
    h_in.wait()
    now = 2
    share = -(-n_norm // (LAG_A + 1 - now))

    def seg_start(i):
        only_a(i)
        norm_into(gain_attn, jnp.minimum((i - 2) * share, n_norm), jnp.minimum((i - 1) * share, n_norm))
    assert n_a > LAG_A + 1 + n_qk + n_v + n_seq * kv_heads // 2 + n_wo
    loop(now, LAG_A + 1, seg_start)
    now = LAG_A + 1
    load_copy_a(0).start()

    def seg_qk(i):
        only_a(i + LAG_A + 1)
        project(i, True)

    def seg_v(i):
        only_a(i + LAG_A + 1)
        project(i, False)
    loop(0, n_qk, seg_qk)
    loop(n_qk, n_qk + n_v, seg_v)
    now += n_qk + n_v
    att_from = now

    def seg_att(i):
        only_a(att_from + i)
        attend(2 * i)
        attend(2 * i + 1)
    n_att = n_seq * kv_heads // 2
    loop(0, n_att, seg_att)
    now += n_att
    wo_from = now

    def seg_wo(i):
        only_a(wo_from + i)
        project_out(i)
    loop(0, n_wo, seg_wo)
    now += n_wo
    norm_into(gain_mlp, 0, n_norm)
    rounds = n_gu // 4
    need = max(first_gu + 4 * i + 4 + LAG_A - (3 * i + 2) for i in range(rounds))
    if now < need:
        loop(now, need, tick)
        now = need
    gu_from = now

    def seg_gu(i):
        t = gu_from + 3 * i
        tick(t)
        gate_up(4 * i)
        tick(t + 1)
        gate_up(4 * i + 1)
        tick(t + 2)
        gate_up(4 * i + 2)
        gate_up(4 * i + 3)
    loop(0, rounds, seg_gu)
    now += 3 * rounds
    need = n_a + max(LAG_A, LAG_B + 1)
    if now < need:
        loop(now, need, tick)
        now = need
    only_b = functools.partial(tick, may_a=False)
    pairs = min(now - n_a - LAG_B - 1, n_b // 2)
    pair_from, one_from = now, now + pairs

    def seg_pair(i):
        only_b(pair_from + i)
        down(2 * i)
        down(2 * i + 1)
    loop(0, pairs, seg_pair)

    def seg_one(i):
        only_b(one_from + i)
        down(2 * pairs + i)
    loop(0, n_b - 2 * pairs, seg_one)
    assert one_from + n_b - 2 * pairs >= n_a + n_b + LAG_B

    loop(0, n_a, ga.drain)
    loop(0, n_b, gb.drain)
    put_out(n_b // 2 - 1)
    pltpu.make_async_copy(h_s, out_ref, io_sem.at[1]).wait()


def norm_kernel(h_ref, gain, out_ref):
    out_ref[...] = rms_norm(h_ref[...], gain[...])


def final_norm(h, gain):
    n_tok, width = h.shape
    rows = min(128, n_tok)
    spec = pl.BlockSpec((rows, width), lambda i: (i, 0))
    return pl.pallas_call(
        norm_kernel, grid=(n_tok // rows,), in_specs=[spec, pl.BlockSpec((1, width), lambda i: (0, 0))], out_specs=spec,
        out_shape=jax.ShapeDtypeStruct((n_tok, width), jnp.bfloat16), name='final_norm',
        cost_estimate=pl.CostEstimate(flops=6 * n_tok * width, bytes_accessed=4 * n_tok * width, transcendentals=n_tok),
    )(h, gain[None])


def run_layer(h0, cos, sin, gain_attn, gain_mlp, w_query, w_key, w_value, w_out, w_gate, w_up, w_down, n_dev, n_seq):
    n_tok, width = h0.shape
    rows, n_heads, head_dim = w_query.shape
    kv_heads = w_key.shape[1]
    seq_len = n_tok // n_seq
    ff = w_gate.shape[1]
    rows_b = w_down.shape[0]
    w_q, w_k, w_v = (w.reshape(rows, -1) for w in (w_query, w_key, w_value))
    n_a = (w_q.shape[1] + w_k.shape[1] + w_v.shape[1] + width) // (2 * COLS) + ff // COLS
    n_b = 2 * (width // COLS)
    chips = n_dev // 2
    any_spec = pl.BlockSpec(memory_space=pl.ANY)
    vmem_spec = pl.BlockSpec(memory_space=pltpu.VMEM)
    n_weights = n_dev * (n_a * rows * 2 * COLS + rows_b * width)
    operands = (h0, w_q, w_k, w_v, w_out, w_gate, w_up, w_down, cos, sin, gain_attn[None], gain_mlp[None])
    out, _, _ = pl.pallas_call(
        functools.partial(layer_kernel, (n_seq, seq_len, n_heads, kv_heads, head_dim)),
        out_shape=(
            jax.ShapeDtypeStruct((n_tok, width), jnp.bfloat16),
            jax.ShapeDtypeStruct((n_a, chips, 2, 2, rows, COLS), jnp.bfloat16),
            jax.ShapeDtypeStruct((n_b, chips, 2, 2, rows_b // 4, COLS), jnp.bfloat16),
        ),
        in_specs=[any_spec] * 8 + [vmem_spec] * (len(operands) - 8),
        out_specs=(any_spec,) * 3,
        scratch_shapes=[
            pltpu.VMEM((n_tok, width), jnp.bfloat16),
            pltpu.VMEM((n_tok, width), jnp.bfloat16),
            pltpu.VMEM((n_heads + 2 * kv_heads, n_tok, head_dim), jnp.bfloat16),
            pltpu.VMEM((2, n_tok, ff // 2), jnp.bfloat16),
            pltpu.VMEM((n_tok, COLS), jnp.float32),
            pltpu.VMEM((2, chips, 2, 2, rows, COLS), jnp.bfloat16),
            pltpu.VMEM((2, chips, 2, 2, rows_b // 4, COLS), jnp.bfloat16),
            pltpu.SemaphoreType.DMA((n_a, N_RECV)),
            pltpu.SemaphoreType.DMA((n_b, N_RECV)),
            pltpu.SemaphoreType.DMA((n_a,)),
            pltpu.SemaphoreType.DMA((n_b,)),
            pltpu.SemaphoreType.DMA((n_a,)),
            pltpu.SemaphoreType.DMA((n_b,)),
            pltpu.SemaphoreType.DMA((2,)),
            pltpu.SemaphoreType.DMA((2,)),
            pltpu.SemaphoreType.DMA((2,)),
        ],
        compiler_params=pltpu.CompilerParams(
            collective_id=0, has_side_effects=True, vmem_limit_bytes=66_000_000),
        cost_estimate=pl.CostEstimate(flops=2 * n_tok * n_weights, bytes_accessed=4 * n_weights, transcendentals=0),
        name='prefill_layer',
    )(*operands)
    return out


def solution(mesh):
    token_spec = P(('data', 'wg'))
    weight_spec = P(None, 'wg')
    whole_spec = P()
    in_specs = (token_spec, token_spec, whole_spec, whole_spec, weight_spec, weight_spec, weight_spec, weight_spec, weight_spec, weight_spec, weight_spec, whole_spec)
    n_dev = mesh.shape['wg']
    assert n_dev == 2 * RING * RING

    def local_forward(h0, positions, norm_attn, norm_mlp, w_query, w_key, w_value, w_out, w_gate, w_up, w_down, norm_final):
        cos, sin = rope_tables(positions.reshape(-1), w_query.shape[-1])
        residual = h0.reshape(-1, h0.shape[-1])
        for l in range(w_query.shape[0]):
            residual = run_layer(residual, cos, sin, norm_attn[l], norm_mlp[l], w_query[l], w_key[l], w_value[l],
                                 w_out[l], w_gate[l], w_up[l], w_down[l], n_dev, h0.shape[0])
        return final_norm(residual, norm_final).reshape(h0.shape)

    return jax.shard_map(local_forward, mesh=mesh, in_specs=in_specs, out_specs=token_spec, check_vma=False)
```

```python
import functools
import math

import jax
import jax.numpy as jnp
from jax import lax
from jax.experimental import pallas as pl
from jax.experimental.pallas import tpu as pltpu
from jax.sharding import PartitionSpec as P

EPS = 1e-5
ROPE_BASE = 10000.0
COLS = 256
LAGS_A = (0, 2, 4, 6, 8, 9)
LAGS_B = (0, 1, 2, 3, 4, 5)
LAG_A, LAG_B = LAGS_A[-1], LAGS_B[-1]
RING = 4
AHEAD = 3
MESH = pl.DeviceIdType.MESH

R_M0, R_P0, R_20, R_0M, R_MM, R_PP, R_2P, R_REST, R_TWIN, R_OWN = range(10)
N_RECV = 10
N_REST = 8


def rms_norm(values_in, gain_vec):
    as_f32 = values_in.astype(jnp.float32)
    mean_sq = jnp.mean(as_f32 * as_f32, axis=-1, keepdims=True)
    return (as_f32 * lax.rsqrt(mean_sq + EPS) * gain_vec).astype(jnp.bfloat16)


def rope_tables(positions, head_dim):
    half_dim = head_dim // 2
    n_seq, seq_len = positions.shape
    lane = jnp.arange(head_dim)
    exponents = (lane % half_dim).astype(jnp.float32) * (2.0 / head_dim)
    inv_freq = jnp.power(jnp.float32(ROPE_BASE), -exponents)
    pairs = positions.astype(jnp.float32).reshape(n_seq // 2, 2, seq_len, 1)
    angles = jnp.where(lane < half_dim, pairs[:, 0], pairs[:, 1]) * inv_freq
    return tuple(f(angles).reshape(-1, head_dim) for f in (jnp.cos, jnp.sin))


class Place:
    def __init__(self):
        me = lax.axis_index('wg')
        self.core = lax.rem(me, 2)
        chip = me // 2
        col, row = lax.rem(chip, RING), chip // RING
        at = lambda dc, dr: lax.rem(row + dr + RING, RING) * RING + lax.rem(col + dc + RING, RING)
        self.at = {(i, j): at(i, j) for i in (-1, 0, 1, 2) for j in (-1, 0, 1, 2)}
        self.near = tuple(self.at[rel] * 2 + self.core for rel in ((1, 0), (-1, 0), (0, 1), (0, -1)))
        self.twin = chip * 2 + 1 - self.core
        self.me = me

    def chip(self, blk, rel):
        straight, turned = self.at[rel], self.at[rel[::-1]]
        return straight + lax.rem(blk + self.core, 2) * (turned - straight)

    def dev(self, blk, dp, ds):
        return self.chip(blk, (dp, ds)) * 2 + self.core


class Gather:
    def __init__(self, place, own, full, recv, send, twin_send):
        self.pl, self.own, self.full = place, own, full
        self.recv, self.send_sem, self.twin_send = recv, send, twin_send

    def spot(self, blk, rel, part=None):
        ref = self.full.at[blk, self.pl.chip(blk, rel), self.pl.core]
        return ref if part is None else ref.at[part]

    def copy(self, blk, src, dst, r, dev):
        return pltpu.make_async_remote_copy(
            src_ref=src, dst_ref=dst, send_sem=self.send_sem.at[blk],
            recv_sem=self.recv.at[blk, r], device_id={'wg': dev}, device_id_type=MESH)

    def put(self, blk, rel, r, dev, part=None):
        ref = self.spot(blk, rel, part)
        self.copy(blk, ref, ref, r, dev).start()

    def got(self, blk, rel, r, part=None):
        ref = self.spot(blk, rel, part)
        self.copy(blk, ref, ref, r, self.pl.me).wait_recv()

    def place_own(self, blk):
        for lo, hi, own in self.own:
            def start():
                for part in range(2):
                    pltpu.make_async_copy(own(blk, part), self.spot(blk, (0, 0), part), self.recv.at[blk, R_OWN]).start()
            if len(self.own) == 1:
                start()
            elif lo < hi:
                pl.when(jnp.logical_and(blk >= lo, blk < hi))(start)

    def take(self, blk, r, n_chunks):
        ref = self.full.at[blk, pl.ds(0, n_chunks), 0]
        pltpu.make_async_copy(ref, ref, self.recv.at[blk, r]).wait()

    def twin_copy(self, blk, core):
        ref = self.full.at[blk, :, core]
        return pltpu.make_async_remote_copy(
            src_ref=ref, dst_ref=ref, send_sem=self.twin_send.at[blk],
            recv_sem=self.recv.at[blk, R_TWIN], device_id={'wg': self.pl.twin}, device_id_type=MESH)

    def stage(self, step, blk):
        w, got, put = self.pl, self.got, self.put
        p_up, p_dn, s_up, s_dn = (w.dev(blk, *rel) for rel in ((1, 0), (-1, 0), (0, 1), (0, -1)))
        own = (0, 0)
        if step == 0:
            self.take(blk, R_OWN, 1)
            put(blk, own, R_M0, p_up)
            put(blk, own, R_P0, p_dn)
            put(blk, own, R_0M, s_up)
            put(blk, own, R_REST, s_dn)
        elif step == 1:
            got(blk, (-1, 0), R_M0)
            put(blk, (-1, 0), R_20, p_up, 0)
            put(blk, (-1, 0), R_MM, s_up)
            put(blk, (-1, 0), R_REST, s_dn)
            got(blk, (1, 0), R_P0)
            put(blk, (1, 0), R_20, p_dn, 1)
            put(blk, (1, 0), R_REST, s_up)
            put(blk, (1, 0), R_PP, s_dn)
            got(blk, (0, -1), R_0M)
            put(blk, (0, -1), R_REST, s_up)
        elif step == 2:
            got(blk, (2, 0), R_20)
            put(blk, (2, 0), R_REST, s_up)
            put(blk, (2, 0), R_2P, s_dn)
            got(blk, (-1, -1), R_MM)
            put(blk, (-1, -1), R_REST, s_up)
            got(blk, (1, 1), R_PP)
            put(blk, (1, 1), R_REST, s_dn)
        elif step == 3:
            got(blk, (2, 1), R_2P)
            put(blk, (2, 1), R_REST, s_dn)
        elif step == 4:
            self.take(blk, R_REST, N_REST)
            self.twin_copy(blk, w.core).start()
        else:
            self.twin_copy(blk, 1 - w.core).wait_recv()

    def drain(self, blk):
        whole = self.full.at[blk, pl.ds(0, RING * RING - 1), 0]
        pltpu.make_async_copy(whole, whole, self.send_sem.at[blk]).wait()
        self.twin_copy(blk, self.pl.core).wait_send()


def layer_kernel(dims, h0, w_q, w_k, w_v, w_o, w_g, w_u, w_d, cos2, sin2, gain_attn, gain_mlp, out_ref, full_a, full_b,
                 h_s, a_s, heads, u_s, acc_s, cos, sin, buf_a, buf_b, recv_a, recv_b, send_a, send_b, twin_a, twin_b, load_a, load_b, io_sem):
    n_seq, seq_len, n_heads, kv_heads, head_dim = dims
    n_tok, width = h_s.shape
    n_rep = n_heads // kv_heads
    blk_cols = 2 * COLS
    per_part = COLS // head_dim
    n_q, n_k = n_heads * head_dim // blk_cols, kv_heads * head_dim // blk_cols
    n_qk, n_v = n_q + n_k, n_k
    n_wo = width // blk_cols
    n_gu = w_g.shape[1] // COLS
    first_gu = n_qk + n_v + n_wo
    n_a = first_gu + n_gu
    rows_b = w_d.shape[0]
    half_b = rows_b // 2
    n_b = 2 * (width // COLS)
    place = Place()

    def cols_of(ref, blk, part):
        return ref.at[:, pl.ds(pl.multiple_of((2 * blk + part) * COLS, COLS), COLS)]

    def ff_cols(blk, part):
        return (w_g, w_u)[part].at[:, pl.ds(pl.multiple_of((blk - first_gu) * COLS, COLS), COLS)]

    def down_part(blk, part):
        quarter = half_b // 2
        return w_d.at[pl.ds(pl.multiple_of(lax.rem(blk, 2) * half_b + part * quarter, quarter), quarter),
                      pl.ds(pl.multiple_of(blk // 2 * COLS, COLS), COLS)]
    own_a = [(0, n_q, lambda blk, part: cols_of(w_q, blk, part)),
             (n_q, n_qk, lambda blk, part: cols_of(w_k, blk - n_q, part)),
             (n_qk, n_qk + n_v, lambda blk, part: cols_of(w_v, blk - n_qk, part)),
             (n_qk + n_v, first_gu, lambda blk, part: cols_of(w_o, blk - n_qk - n_v, part)),
             (first_gu, n_a, ff_cols)]
    ga = Gather(place, own_a, full_a, recv_a, send_a, twin_a)
    gb = Gather(place, [(0, n_b, down_part)], full_b, recv_b, send_b, twin_b)

    for blk in range(AHEAD):
        ga.place_own(jnp.int32(blk))
    barrier = pltpu.get_barrier_semaphore()
    near = place.near + (place.twin,)
    for dev in near:
        pl.semaphore_signal(barrier, inc=1, device_id={'wg': dev}, device_id_type=MESH)
    pl.semaphore_wait(barrier, len(near))

    def place_ahead(blk, may_a, may_b):
        if may_a:
            @pl.when(blk < n_a)
            def _():
                ga.place_own(blk)
        if may_b:
            @pl.when(jnp.logical_and(blk >= n_a, blk < n_a + n_b))
            def _():
                gb.place_own(blk - n_a)

    def tick(t, may_a=True, may_b=True):
        place_ahead(t + AHEAD, may_a, may_b)
        for step, (lag_a, lag_b) in enumerate(zip(LAGS_A, LAGS_B)):
            if may_a:
                @pl.when(jnp.logical_and(t - lag_a >= 0, t - lag_a < n_a))
                def _():
                    ga.stage(step, t - lag_a)
            if may_b:
                @pl.when(jnp.logical_and(t - lag_b >= n_a, t - lag_b < n_a + n_b))
                def _():
                    gb.stage(step, t - lag_b - n_a)

    def load_copy_a(i):
        slot = lax.rem(i, 2)
        return pltpu.make_async_copy(full_a.at[i], buf_a.at[slot], load_a.at[slot])

    def load_copy_b(i):
        slot = lax.rem(i, 2)
        return pltpu.make_async_copy(full_b.at[i], buf_b.at[slot], load_b.at[slot])

    def weights_a(i, part):
        return buf_a[lax.rem(i, 2), :, :, part].reshape(width, COLS)

    def weights_b(i):
        return buf_b[lax.rem(i, 2)].reshape(-1, COLS)

    def dot(x, w):
        return jnp.dot(x, w, preferred_element_type=jnp.float32)

    norm_rows = min(64, seq_len)

    def norm_into(gain, lo, hi):
        def body(i, _):
            sl = pl.ds(pl.multiple_of(i * norm_rows, norm_rows), norm_rows)
            a_s[sl, :] = rms_norm(h_s[sl, :], gain[...])
            return 0
        lax.fori_loop(lo, hi, body, 0)

    def over_seqs(body):
        def step(b, _):
            body(pl.ds(pl.multiple_of(b * seq_len, seq_len), seq_len))
            return 0
        lax.fori_loop(0, n_seq, step, 0)

    def project(i, rope):
        load_copy_a(i).wait()
        load_copy_a(i + 1).start()

        def body(rows):
            for part in range(2):
                out = dot(a_s[rows, :], weights_a(i, part)).astype(jnp.bfloat16)
                for j in range(per_part):
                    one = out[:, j * head_dim:(j + 1) * head_dim]
                    if rope:
                        one = one.astype(jnp.float32)
                        one = (one * cos[rows, :] + pltpu.roll(one, head_dim // 2, 1) * sin[rows, :]).astype(jnp.bfloat16)
                    heads[(2 * i + part) * per_part + j, rows, :] = one
        over_seqs(body)

    q_block = seq_len // 2

    def attend(n):
        seq, group = n // kv_heads, lax.rem(n, kv_heads)
        start = pl.multiple_of(seq * seq_len, seq_len)
        for qb in range(2):
            n_keys = (qb + 1) * q_block
            keys = heads[n_heads + group, pl.ds(start, n_keys), :]
            vals = heads[n_heads + kv_heads + group, pl.ds(start, n_keys), :]
            q_rows = pl.ds(pl.multiple_of(start + qb * q_block, q_block), q_block)
            q_idx = qb * q_block + lax.broadcasted_iota(jnp.int32, (q_block, n_keys), 0)
            k_idx = lax.broadcasted_iota(jnp.int32, (q_block, n_keys), 1)
            for r in range(n_rep):
                head = group * n_rep + r
                scores = lax.dot_general(heads[head, q_rows, :], keys, (((1,), (1,)), ((), ())),
                                         preferred_element_type=jnp.float32) * head_dim ** -0.5
                scores = jnp.where(k_idx <= q_idx, scores, -1e30)
                top = jnp.max(scores, axis=-1, keepdims=True)
                expd = jnp.exp(scores - top)
                total = jnp.sum(expd, axis=-1, keepdims=True)
                probs = (expd / total).astype(jnp.bfloat16)
                cols = pl.ds(pl.multiple_of(head * head_dim, head_dim), head_dim)
                a_s[q_rows, cols] = dot(probs, vals).astype(jnp.bfloat16)

    def project_out(i):
        blk = n_qk + n_v + i
        load_copy_a(blk).wait()
        load_copy_a(blk + 1).start()

        def body(rows):
            for part in range(2):
                cols = pl.ds(pl.multiple_of((2 * i + part) * COLS, COLS), COLS)
                out = dot(a_s[rows, :], weights_a(blk, part))
                h_s[rows, cols] = (h_s[rows, cols].astype(jnp.float32) + out).astype(jnp.bfloat16)
        over_seqs(body)

    def gate_up(i):
        blk = first_gu + i
        load_copy_a(blk).wait()

        @pl.when(i + 1 < n_gu)
        def _():
            load_copy_a(blk + 1).start()

        @pl.when(i + 1 == n_gu)
        def _():
            load_copy_b(0).start()
        n_own = COLS // rows_b

        def body(rows):
            gate = dot(a_s[rows, :], weights_a(blk, 0))
            up = dot(a_s[rows, :], weights_a(blk, 1))
            u = (gate * jax.nn.sigmoid(gate) * up).astype(jnp.bfloat16)
            for j in range(n_own):
                to = pl.ds(pl.multiple_of((i * n_own + j) * half_b, half_b), half_b)
                for half in range(2):
                    u_s[half, rows, to] = u[:, j * rows_b + half * half_b:j * rows_b + (half + 1) * half_b]
        over_seqs(body)

    def down(i):
        load_copy_b(i).wait()

        @pl.when(i + 1 < n_b)
        def _():
            load_copy_b(i + 1).start()
        cols = pl.ds(pl.multiple_of(i // 2 * COLS, COLS), COLS)

        def first_half(rows):
            acc_s[rows, :] = dot(u_s[0, rows, :], weights_b(i))

        def second_half(rows):
            out = acc_s[rows, :] + dot(u_s[1, rows, :], weights_b(i))
            h_s[rows, cols] = (h_s[rows, cols].astype(jnp.float32) + out).astype(jnp.bfloat16)

        @pl.when(lax.rem(i, 2) == 0)
        def _():
            over_seqs(first_half)

            @pl.when(i > 0)
            def _():
                put_out(i // 2 - 1)

        @pl.when(lax.rem(i, 2) == 1)
        def _():
            over_seqs(second_half)

    def put_out(j):
        cols = pl.ds(pl.multiple_of(j * COLS, COLS), COLS)
        pltpu.make_async_copy(h_s.at[:, cols], out_ref.at[:, cols], io_sem.at[1]).start()

    def loop(lo, hi, body):
        def step(i, _):
            body(i)
            return 0
        lax.fori_loop(lo, hi, step, 0)

    h_in = pltpu.make_async_copy(h0, h_s, io_sem.at[0])
    h_in.start()
    only_a = functools.partial(tick, may_b=False)
    n_norm = n_tok // norm_rows
    only_a(0)
    only_a(1)
    h_in.wait()
    now = 2
    share = -(-n_norm // (LAG_A + 1 - now))

    half_dim = head_dim // 2

    def spread(i):
        table = pl.ds(pl.multiple_of(i * seq_len, seq_len), seq_len)
        low = lax.broadcasted_iota(jnp.int32, (seq_len, head_dim), 1) < half_dim
        c, s = cos2[table, :], sin2[table, :]
        c_turned, s_turned = pltpu.roll(c, half_dim, 1), pltpu.roll(s, half_dim, 1)
        for j, (c_j, s_j) in enumerate(((jnp.where(low, c, c_turned), jnp.where(low, -s, s_turned)),
                                        (jnp.where(low, c_turned, c), jnp.where(low, -s_turned, s)))):
            rows = pl.ds(pl.multiple_of((2 * i + j) * seq_len, seq_len), seq_len)
            cos[rows, :] = c_j
            sin[rows, :] = s_j
    loop(0, n_seq // 2, spread)

    def seg_start(i):
        only_a(i)
        norm_into(gain_attn, jnp.minimum((i - 2) * share, n_norm), jnp.minimum((i - 1) * share, n_norm))
    assert n_a > LAG_A + 1 + n_qk + n_v + n_seq * kv_heads // 2 + n_wo
    loop(now, LAG_A + 1, seg_start)
    now = LAG_A + 1
    load_copy_a(0).start()

    def seg_qk(i):
        only_a(i + LAG_A + 1)
        project(i, True)

    def seg_v(i):
        only_a(i + LAG_A + 1)
        project(i, False)
    loop(0, n_qk, seg_qk)
    loop(n_qk, n_qk + n_v, seg_v)
    now += n_qk + n_v
    att_from = now

    def seg_att(i):
        only_a(att_from + i)
        attend(2 * i)
        attend(2 * i + 1)
    n_att = n_seq * kv_heads // 2
    loop(0, n_att, seg_att)
    now += n_att
    wo_from = now

    def seg_wo(i):
        only_a(wo_from + i)
        project_out(i)
    loop(0, n_wo, seg_wo)
    now += n_wo
    norm_into(gain_mlp, 0, n_norm)
    rounds = n_gu // 4
    need = max(first_gu + 4 * i + 4 + LAG_A - (3 * i + 2) for i in range(rounds))
    if now < need:
        loop(now, need, tick)
        now = need
    gu_from = now

    def seg_gu(i):
        t = gu_from + 3 * i
        tick(t)
        gate_up(4 * i)
        tick(t + 1)
        gate_up(4 * i + 1)
        tick(t + 2)
        gate_up(4 * i + 2)
        gate_up(4 * i + 3)
    loop(0, rounds, seg_gu)
    now += 3 * rounds
    need = n_a + max(LAG_A, LAG_B + 1)
    if now < need:
        loop(now, need, tick)
        now = need
    only_b = functools.partial(tick, may_a=False)
    pairs = min(now - n_a - LAG_B - 1, n_b // 2)
    pair_from, one_from = now, now + pairs

    def seg_pair(i):
        only_b(pair_from + i)
        down(2 * i)
        down(2 * i + 1)
    loop(0, pairs, seg_pair)
    loop(0, n_a, ga.drain)

    def seg_one(i):
        only_b(one_from + i)
        down(2 * pairs + i)
    loop(0, n_b - 2 * pairs, seg_one)
    assert one_from + n_b - 2 * pairs >= n_a + n_b + LAG_B

    loop(0, n_b, gb.drain)
    put_out(n_b // 2 - 1)
    pltpu.make_async_copy(h_s, out_ref, io_sem.at[1]).wait()


def norm_kernel(h_ref, gain, out_ref):
    out_ref[...] = rms_norm(h_ref[...], gain[...])


def final_norm(h, gain):
    n_tok, width = h.shape
    rows = min(128, n_tok)
    spec = pl.BlockSpec((rows, width), lambda i: (i, 0))
    return pl.pallas_call(
        norm_kernel, grid=(n_tok // rows,), in_specs=[spec, pl.BlockSpec((1, width), lambda i: (0, 0))], out_specs=spec,
        out_shape=jax.ShapeDtypeStruct((n_tok, width), jnp.bfloat16), name='final_norm',
        cost_estimate=pl.CostEstimate(flops=6 * n_tok * width, bytes_accessed=4 * n_tok * width, transcendentals=n_tok),
    )(h, gain[None])


def run_layer(h0, cos, sin, gain_attn, gain_mlp, w_query, w_key, w_value, w_out, w_gate, w_up, w_down, n_dev, n_seq):
    n_tok, width = h0.shape
    rows, n_heads, head_dim = w_query.shape
    kv_heads = w_key.shape[1]
    seq_len = n_tok // n_seq
    ff = w_gate.shape[1]
    rows_b = w_down.shape[0]
    w_q, w_k, w_v = (w.reshape(rows, -1) for w in (w_query, w_key, w_value))
    n_a = (w_q.shape[1] + w_k.shape[1] + w_v.shape[1] + width) // (2 * COLS) + ff // COLS
    n_b = 2 * (width // COLS)
    chips = n_dev // 2
    any_spec = pl.BlockSpec(memory_space=pl.ANY)
    vmem_spec = pl.BlockSpec(memory_space=pltpu.VMEM)
    n_weights = n_dev * (n_a * rows * 2 * COLS + rows_b * width)
    operands = (h0, w_q, w_k, w_v, w_out, w_gate, w_up, w_down, cos, sin, gain_attn[None], gain_mlp[None])
    out, _, _ = pl.pallas_call(
        functools.partial(layer_kernel, (n_seq, seq_len, n_heads, kv_heads, head_dim)),
        out_shape=(
            jax.ShapeDtypeStruct((n_tok, width), jnp.bfloat16),
            jax.ShapeDtypeStruct((n_a, chips, 2, 2, rows, COLS), jnp.bfloat16),
            jax.ShapeDtypeStruct((n_b, chips, 2, 2, rows_b // 4, COLS), jnp.bfloat16),
        ),
        in_specs=[any_spec] * 8 + [vmem_spec] * (len(operands) - 8),
        out_specs=(any_spec,) * 3,
        scratch_shapes=[
            pltpu.VMEM((n_tok, width), jnp.bfloat16),
            pltpu.VMEM((n_tok, width), jnp.bfloat16),
            pltpu.VMEM((n_heads + 2 * kv_heads, n_tok, head_dim), jnp.bfloat16),
            pltpu.VMEM((2, n_tok, ff // 2), jnp.bfloat16),
            pltpu.VMEM((n_tok, COLS), jnp.float32),
            pltpu.VMEM((n_tok, head_dim), jnp.float32),
            pltpu.VMEM((n_tok, head_dim), jnp.float32),
            pltpu.VMEM((2, chips, 2, 2, rows, COLS), jnp.bfloat16),
            pltpu.VMEM((2, chips, 2, 2, rows_b // 4, COLS), jnp.bfloat16),
            pltpu.SemaphoreType.DMA((n_a, N_RECV)),
            pltpu.SemaphoreType.DMA((n_b, N_RECV)),
            pltpu.SemaphoreType.DMA((n_a,)),
            pltpu.SemaphoreType.DMA((n_b,)),
            pltpu.SemaphoreType.DMA((n_a,)),
            pltpu.SemaphoreType.DMA((n_b,)),
            pltpu.SemaphoreType.DMA((2,)),
            pltpu.SemaphoreType.DMA((2,)),
            pltpu.SemaphoreType.DMA((2,)),
        ],
        compiler_params=pltpu.CompilerParams(
            collective_id=0, has_side_effects=True, vmem_limit_bytes=66_000_000),
        cost_estimate=pl.CostEstimate(flops=2 * n_tok * n_weights, bytes_accessed=4 * n_weights, transcendentals=0),
        name='prefill_layer',
    )(*operands)
    return out


def solution(mesh):
    token_spec = P(('data', 'wg'))
    weight_spec = P(None, 'wg')
    whole_spec = P()
    in_specs = (token_spec, token_spec, whole_spec, whole_spec, weight_spec, weight_spec, weight_spec, weight_spec, weight_spec, weight_spec, weight_spec, whole_spec)
    n_dev = mesh.shape['wg']
    assert n_dev == 2 * RING * RING

    def local_forward(h0, positions, norm_attn, norm_mlp, w_query, w_key, w_value, w_out, w_gate, w_up, w_down, norm_final):
        cos, sin = rope_tables(positions, w_query.shape[-1])
        residual = h0.reshape(-1, h0.shape[-1])
        for l in range(w_query.shape[0]):
            residual = run_layer(residual, cos, sin, norm_attn[l], norm_mlp[l], w_query[l], w_key[l], w_value[l],
                                 w_out[l], w_gate[l], w_up[l], w_down[l], n_dev, h0.shape[0])
        return final_norm(residual, norm_final).reshape(h0.shape)

    return jax.shard_map(local_forward, mesh=mesh, in_specs=in_specs, out_specs=token_spec, check_vma=False)
```

```python
import functools
import math

import jax
import jax.numpy as jnp
from jax import lax
from jax.experimental import pallas as pl
from jax.experimental.pallas import tpu as pltpu
from jax.sharding import PartitionSpec as P

EPS = 1e-5
ROPE_BASE = 10000.0
COLS = 256
LAGS_A = (0, 2, 4, 6, 8, 9)
LAGS_B = (0, 1, 2, 3, 5, 6)
LAG_A, LAG_B = LAGS_A[-1], LAGS_B[-1]
RING = 4
AHEAD = 3
MESH = pl.DeviceIdType.MESH

R_M0, R_P0, R_20, R_0M, R_MM, R_PP, R_2P, R_REST, R_TWIN, R_OWN = range(10)
N_RECV = 10
N_REST = 8


def rms_norm(values_in, gain_vec):
    as_f32 = values_in.astype(jnp.float32)
    mean_sq = jnp.mean(as_f32 * as_f32, axis=-1, keepdims=True)
    return (as_f32 * lax.rsqrt(mean_sq + EPS) * gain_vec).astype(jnp.bfloat16)


def rope_tables(positions, head_dim):
    half_dim = head_dim // 2
    n_seq, seq_len = positions.shape
    lane = jnp.arange(head_dim)
    exponents = (lane % half_dim).astype(jnp.float32) * (2.0 / head_dim)
    inv_freq = jnp.power(jnp.float32(ROPE_BASE), -exponents)
    pairs = positions.astype(jnp.float32).reshape(n_seq // 2, 2, seq_len, 1)
    angles = jnp.where(lane < half_dim, pairs[:, 0], pairs[:, 1]) * inv_freq
    return tuple(f(angles).reshape(-1, head_dim) for f in (jnp.cos, jnp.sin))


class Place:
    def __init__(self):
        me = lax.axis_index('wg')
        self.core = lax.rem(me, 2)
        chip = me // 2
        col, row = lax.rem(chip, RING), chip // RING
        at = lambda dc, dr: lax.rem(row + dr + RING, RING) * RING + lax.rem(col + dc + RING, RING)
        self.at = {(i, j): at(i, j) for i in (-1, 0, 1, 2) for j in (-1, 0, 1, 2)}
        self.near = tuple(self.at[rel] * 2 + self.core for rel in ((1, 0), (-1, 0), (0, 1), (0, -1)))
        self.twin = chip * 2 + 1 - self.core
        self.me = me

    def chip(self, blk, rel):
        straight, turned = self.at[rel], self.at[rel[::-1]]
        return straight + lax.rem(blk + self.core, 2) * (turned - straight)

    def dev(self, blk, dp, ds):
        return self.chip(blk, (dp, ds)) * 2 + self.core


class Gather:
    def __init__(self, place, own, full, recv, send, twin_send):
        self.pl, self.own, self.full = place, own, full
        self.recv, self.send_sem, self.twin_send = recv, send, twin_send

    def spot(self, blk, rel, part=None):
        ref = self.full.at[blk, self.pl.chip(blk, rel), self.pl.core]
        return ref if part is None else ref.at[part]

    def copy(self, blk, src, dst, r, dev):
        return pltpu.make_async_remote_copy(
            src_ref=src, dst_ref=dst, send_sem=self.send_sem.at[blk],
            recv_sem=self.recv.at[blk, r], device_id={'wg': dev}, device_id_type=MESH)

    def put(self, blk, rel, r, dev, part=None):
        ref = self.spot(blk, rel, part)
        self.copy(blk, ref, ref, r, dev).start()

    def got(self, blk, rel, r, part=None):
        ref = self.spot(blk, rel, part)
        self.copy(blk, ref, ref, r, self.pl.me).wait_recv()

    def place_own(self, blk):
        for lo, hi, own in self.own:
            def start():
                for part in range(2):
                    pltpu.make_async_copy(own(blk, part), self.spot(blk, (0, 0), part), self.recv.at[blk, R_OWN]).start()
            if len(self.own) == 1:
                start()
            elif lo < hi:
                pl.when(jnp.logical_and(blk >= lo, blk < hi))(start)

    def take(self, blk, r, n_chunks):
        ref = self.full.at[blk, pl.ds(0, n_chunks), 0]
        pltpu.make_async_copy(ref, ref, self.recv.at[blk, r]).wait()

    def twin_copy(self, blk, core):
        ref = self.full.at[blk, :, core]
        return pltpu.make_async_remote_copy(
            src_ref=ref, dst_ref=ref, send_sem=self.twin_send.at[blk],
            recv_sem=self.recv.at[blk, R_TWIN], device_id={'wg': self.pl.twin}, device_id_type=MESH)

    def stage(self, step, blk):
        w, got, put = self.pl, self.got, self.put
        p_up, p_dn, s_up, s_dn = (w.dev(blk, *rel) for rel in ((1, 0), (-1, 0), (0, 1), (0, -1)))
        own = (0, 0)
        if step == 0:
            self.take(blk, R_OWN, 1)
            put(blk, own, R_M0, p_up)
            put(blk, own, R_P0, p_dn)
            put(blk, own, R_0M, s_up)
            put(blk, own, R_REST, s_dn)
        elif step == 1:
            got(blk, (-1, 0), R_M0)
            put(blk, (-1, 0), R_20, p_up, 0)
            put(blk, (-1, 0), R_MM, s_up)
            put(blk, (-1, 0), R_REST, s_dn)
            got(blk, (1, 0), R_P0)
            put(blk, (1, 0), R_20, p_dn, 1)
            put(blk, (1, 0), R_REST, s_up)
            put(blk, (1, 0), R_PP, s_dn)
            got(blk, (0, -1), R_0M)
            put(blk, (0, -1), R_REST, s_up)
        elif step == 2:
            got(blk, (2, 0), R_20)
            put(blk, (2, 0), R_REST, s_up)
            put(blk, (2, 0), R_2P, s_dn)
            got(blk, (-1, -1), R_MM)
            put(blk, (-1, -1), R_REST, s_up)
            got(blk, (1, 1), R_PP)
            put(blk, (1, 1), R_REST, s_dn)
        elif step == 3:
            got(blk, (2, 1), R_2P)
            put(blk, (2, 1), R_REST, s_dn)
        elif step == 4:
            self.take(blk, R_REST, N_REST)
            self.twin_copy(blk, w.core).start()
        else:
            self.twin_copy(blk, 1 - w.core).wait_recv()

    def drain(self, blk):
        whole = self.full.at[blk, pl.ds(0, RING * RING - 1), 0]
        pltpu.make_async_copy(whole, whole, self.send_sem.at[blk]).wait()
        self.twin_copy(blk, self.pl.core).wait_send()


def layer_kernel(dims, h0, w_q, w_k, w_v, w_o, w_g, w_u, w_d, cos2, sin2, gain_attn, gain_mlp, out_ref, full_a, full_b,
                 h_s, a_s, heads, u_s, acc_s, cos, sin, buf_a, buf_b, recv_a, recv_b, send_a, send_b, twin_a, twin_b, load_a, load_b, io_sem):
    n_seq, seq_len, n_heads, kv_heads, head_dim = dims
    n_tok, width = h_s.shape
    n_rep = n_heads // kv_heads
    blk_cols = 2 * COLS
    per_part = COLS // head_dim
    n_q, n_k = n_heads * head_dim // blk_cols, kv_heads * head_dim // blk_cols
    n_qk, n_v = n_q + n_k, n_k
    n_wo = width // blk_cols
    n_gu = w_g.shape[1] // COLS
    first_gu = n_qk + n_v + n_wo
    n_a = first_gu + n_gu
    rows_b = w_d.shape[0]
    half_b = rows_b // 2
    n_b = 2 * (width // COLS)
    place = Place()

    def cols_of(ref, blk, part):
        return ref.at[:, pl.ds(pl.multiple_of((2 * blk + part) * COLS, COLS), COLS)]

    def ff_cols(blk, part):
        return (w_g, w_u)[part].at[:, pl.ds(pl.multiple_of((blk - first_gu) * COLS, COLS), COLS)]

    def down_part(blk, part):
        quarter = half_b // 2
        return w_d.at[pl.ds(pl.multiple_of(lax.rem(blk, 2) * half_b + part * quarter, quarter), quarter),
                      pl.ds(pl.multiple_of(blk // 2 * COLS, COLS), COLS)]
    own_a = [(0, n_q, lambda blk, part: cols_of(w_q, blk, part)),
             (n_q, n_qk, lambda blk, part: cols_of(w_k, blk - n_q, part)),
             (n_qk, n_qk + n_v, lambda blk, part: cols_of(w_v, blk - n_qk, part)),
             (n_qk + n_v, first_gu, lambda blk, part: cols_of(w_o, blk - n_qk - n_v, part)),
             (first_gu, n_a, ff_cols)]
    ga = Gather(place, own_a, full_a, recv_a, send_a, twin_a)
    gb = Gather(place, [(0, n_b, down_part)], full_b, recv_b, send_b, twin_b)

    for blk in range(AHEAD):
        ga.place_own(jnp.int32(blk))
    barrier = pltpu.get_barrier_semaphore()
    near = place.near + (place.twin,)
    for dev in near:
        pl.semaphore_signal(barrier, inc=1, device_id={'wg': dev}, device_id_type=MESH)
    pl.semaphore_wait(barrier, len(near))

    def place_ahead(blk, may_a, may_b):
        if may_a:
            @pl.when(blk < n_a)
            def _():
                ga.place_own(blk)
        if may_b:
            @pl.when(jnp.logical_and(blk >= n_a, blk < n_a + n_b))
            def _():
                gb.place_own(blk - n_a)

    def tick(t, may_a=True, may_b=True):
        place_ahead(t + AHEAD, may_a, may_b)
        for step, (lag_a, lag_b) in enumerate(zip(LAGS_A, LAGS_B)):
            if may_a:
                @pl.when(jnp.logical_and(t - lag_a >= 0, t - lag_a < n_a))
                def _():
                    ga.stage(step, t - lag_a)
            if may_b:
                @pl.when(jnp.logical_and(t - lag_b >= n_a, t - lag_b < n_a + n_b))
                def _():
                    gb.stage(step, t - lag_b - n_a)

    def load_copy_a(i):
        slot = lax.rem(i, 2)
        return pltpu.make_async_copy(full_a.at[i], buf_a.at[slot], load_a.at[slot])

    def load_copy_b(i):
        slot = lax.rem(i, 2)
        return pltpu.make_async_copy(full_b.at[i], buf_b.at[slot], load_b.at[slot])

    def weights_a(i, part):
        return buf_a[lax.rem(i, 2), :, :, part].reshape(width, COLS)

    def weights_b(i):
        return buf_b[lax.rem(i, 2)].reshape(-1, COLS)

    def dot(x, w):
        return jnp.dot(x, w, preferred_element_type=jnp.float32)

    norm_rows = min(64, seq_len)

    def norm_into(gain, lo, hi):
        def body(i, _):
            sl = pl.ds(pl.multiple_of(i * norm_rows, norm_rows), norm_rows)
            a_s[sl, :] = rms_norm(h_s[sl, :], gain[...])
            return 0
        lax.fori_loop(lo, hi, body, 0)

    def over_seqs(body):
        def step(b, _):
            body(pl.ds(pl.multiple_of(b * seq_len, seq_len), seq_len))
            return 0
        lax.fori_loop(0, n_seq, step, 0)

    def project(i, rope):
        load_copy_a(i).wait()
        load_copy_a(i + 1).start()

        def body(rows):
            for part in range(2):
                out = dot(a_s[rows, :], weights_a(i, part)).astype(jnp.bfloat16)
                for j in range(per_part):
                    one = out[:, j * head_dim:(j + 1) * head_dim]
                    if rope:
                        one = one.astype(jnp.float32)
                        one = (one * cos[rows, :] + pltpu.roll(one, head_dim // 2, 1) * sin[rows, :]).astype(jnp.bfloat16)
                    heads[(2 * i + part) * per_part + j, rows, :] = one
        over_seqs(body)

    q_block = seq_len // 2

    def attend(n):
        seq, group = n // kv_heads, lax.rem(n, kv_heads)
        start = pl.multiple_of(seq * seq_len, seq_len)
        for qb in range(2):
            n_keys = (qb + 1) * q_block
            keys = heads[n_heads + group, pl.ds(start, n_keys), :]
            vals = heads[n_heads + kv_heads + group, pl.ds(start, n_keys), :]
            q_rows = pl.ds(pl.multiple_of(start + qb * q_block, q_block), q_block)
            q_idx = qb * q_block + lax.broadcasted_iota(jnp.int32, (q_block, n_keys), 0)
            k_idx = lax.broadcasted_iota(jnp.int32, (q_block, n_keys), 1)
            for r in range(n_rep):
                head = group * n_rep + r
                scores = lax.dot_general(heads[head, q_rows, :], keys, (((1,), (1,)), ((), ())),
                                         preferred_element_type=jnp.float32) * head_dim ** -0.5
                scores = jnp.where(k_idx <= q_idx, scores, -1e30)
                top = jnp.max(scores, axis=-1, keepdims=True)
                expd = jnp.exp(scores - top)
                total = jnp.sum(expd, axis=-1, keepdims=True)
                probs = (expd / total).astype(jnp.bfloat16)
                cols = pl.ds(pl.multiple_of(head * head_dim, head_dim), head_dim)
                a_s[q_rows, cols] = dot(probs, vals).astype(jnp.bfloat16)

    def project_out(i):
        blk = n_qk + n_v + i
        load_copy_a(blk).wait()
        load_copy_a(blk + 1).start()

        def body(rows):
            for part in range(2):
                cols = pl.ds(pl.multiple_of((2 * i + part) * COLS, COLS), COLS)
                out = dot(a_s[rows, :], weights_a(blk, part))
                h_s[rows, cols] = (h_s[rows, cols].astype(jnp.float32) + out).astype(jnp.bfloat16)
        over_seqs(body)

    def gate_up(i):
        blk = first_gu + i
        load_copy_a(blk).wait()

        @pl.when(i + 1 < n_gu)
        def _():
            load_copy_a(blk + 1).start()

        @pl.when(i + 1 == n_gu)
        def _():
            load_copy_b(0).start()
        n_own = COLS // rows_b

        def body(rows):
            gate = dot(a_s[rows, :], weights_a(blk, 0))
            up = dot(a_s[rows, :], weights_a(blk, 1))
            u = (gate * jax.nn.sigmoid(gate) * up).astype(jnp.bfloat16)
            for j in range(n_own):
                to = pl.ds(pl.multiple_of((i * n_own + j) * half_b, half_b), half_b)
                for half in range(2):
                    u_s[half, rows, to] = u[:, j * rows_b + half * half_b:j * rows_b + (half + 1) * half_b]
        over_seqs(body)

    def down(i):
        load_copy_b(i).wait()

        @pl.when(i + 1 < n_b)
        def _():
            load_copy_b(i + 1).start()
        cols = pl.ds(pl.multiple_of(i // 2 * COLS, COLS), COLS)

        def first_half(rows):
            acc_s[rows, :] = dot(u_s[0, rows, :], weights_b(i))

        def second_half(rows):
            out = acc_s[rows, :] + dot(u_s[1, rows, :], weights_b(i))
            h_s[rows, cols] = (h_s[rows, cols].astype(jnp.float32) + out).astype(jnp.bfloat16)

        @pl.when(lax.rem(i, 2) == 0)
        def _():
            over_seqs(first_half)

            @pl.when(i > 0)
            def _():
                put_out(i // 2 - 1)

        @pl.when(lax.rem(i, 2) == 1)
        def _():
            over_seqs(second_half)

    def put_out(j):
        cols = pl.ds(pl.multiple_of(j * COLS, COLS), COLS)
        pltpu.make_async_copy(h_s.at[:, cols], out_ref.at[:, cols], io_sem.at[1]).start()

    def loop(lo, hi, body):
        def step(i, _):
            body(i)
            return 0
        lax.fori_loop(lo, hi, step, 0)

    h_in = pltpu.make_async_copy(h0, h_s, io_sem.at[0])
    h_in.start()
    only_a = functools.partial(tick, may_b=False)
    n_norm = n_tok // norm_rows
    only_a(0)
    only_a(1)
    h_in.wait()
    now = 2
    share = -(-n_norm // (LAG_A + 1 - now))

    half_dim = head_dim // 2

    def spread(i):
        table = pl.ds(pl.multiple_of(i * seq_len, seq_len), seq_len)
        low = lax.broadcasted_iota(jnp.int32, (seq_len, head_dim), 1) < half_dim
        c, s = cos2[table, :], sin2[table, :]
        c_turned, s_turned = pltpu.roll(c, half_dim, 1), pltpu.roll(s, half_dim, 1)
        for j, (c_j, s_j) in enumerate(((jnp.where(low, c, c_turned), jnp.where(low, -s, s_turned)),
                                        (jnp.where(low, c_turned, c), jnp.where(low, -s_turned, s)))):
            rows = pl.ds(pl.multiple_of((2 * i + j) * seq_len, seq_len), seq_len)
            cos[rows, :] = c_j
            sin[rows, :] = s_j
    loop(0, n_seq // 2, spread)

    def seg_start(i):
        only_a(i)
        norm_into(gain_attn, jnp.minimum((i - 2) * share, n_norm), jnp.minimum((i - 1) * share, n_norm))
    assert n_a > LAG_A + 1 + n_qk + n_v + n_seq * kv_heads // 2 + n_wo
    loop(now, LAG_A + 1, seg_start)
    now = LAG_A + 1
    load_copy_a(0).start()

    def seg_qk(i):
        only_a(i + LAG_A + 1)
        project(i, True)

    def seg_v(i):
        only_a(i + LAG_A + 1)
        project(i, False)
    loop(0, n_qk, seg_qk)
    loop(n_qk, n_qk + n_v, seg_v)
    now += n_qk + n_v
    att_from = now

    def seg_att(i):
        only_a(att_from + i)
        attend(2 * i)
        attend(2 * i + 1)
    n_att = n_seq * kv_heads // 2
    loop(0, n_att, seg_att)
    now += n_att
    wo_from = now

    def seg_wo(i):
        only_a(wo_from + i)
        project_out(i)
    loop(0, n_wo, seg_wo)
    now += n_wo
    norm_into(gain_mlp, 0, n_norm)
    rounds = n_gu // 4
    need = max(first_gu + 4 * i + 4 + LAG_A - (3 * i + 2) for i in range(rounds))
    if now < need:
        loop(now, need, tick)
        now = need
    gu_from = now

    def seg_gu(i):
        t = gu_from + 3 * i
        tick(t)
        gate_up(4 * i)
        tick(t + 1)
        gate_up(4 * i + 1)
        tick(t + 2)
        gate_up(4 * i + 2)
        gate_up(4 * i + 3)
    loop(0, rounds, seg_gu)
    now += 3 * rounds
    need = n_a + max(LAG_A, LAG_B + 1)
    if now < need:
        loop(now, need, tick)
        now = need
    only_b = functools.partial(tick, may_a=False)
    pairs = min(now - n_a - LAG_B - 1, n_b // 2)
    pair_from, one_from = now, now + pairs

    def seg_pair(i):
        only_b(pair_from + i)
        down(2 * i)
        down(2 * i + 1)
    loop(0, pairs, seg_pair)
    loop(0, n_a, ga.drain)

    def seg_one(i):
        only_b(one_from + i)
        down(2 * pairs + i)
    loop(0, n_b - 2 * pairs, seg_one)
    assert one_from + n_b - 2 * pairs >= n_a + n_b + LAG_B

    loop(0, n_b, gb.drain)
    put_out(n_b // 2 - 1)
    pltpu.make_async_copy(h_s, out_ref, io_sem.at[1]).wait()


def norm_kernel(h_ref, gain, out_ref, h_s, out_s, in_sem, out_sem):
    n_part, rows, _ = h_s.shape

    def part_in(i):
        return pltpu.make_async_copy(h_ref.at[pl.ds(i * rows, rows)], h_s.at[i], in_sem.at[i])

    def part_out(i):
        return pltpu.make_async_copy(out_s.at[i], out_ref.at[pl.ds(i * rows, rows)], out_sem.at[i])
    for i in range(n_part):
        part_in(i).start()
    sub = min(64, rows)
    for i in range(n_part):
        part_in(i).wait()

        def body(j, _):
            sl = pl.ds(pl.multiple_of(j * sub, sub), sub)
            out_s[i, sl, :] = rms_norm(h_s[i, sl, :], gain[...])
            return 0
        lax.fori_loop(0, rows // sub, body, 0)
        part_out(i).start()
    for i in range(n_part):
        part_out(i).wait()


def final_norm(h, gain):
    n_tok, width = h.shape
    n_part = 8
    rows = n_tok // n_part
    any_spec = pl.BlockSpec(memory_space=pl.ANY)
    return pl.pallas_call(
        norm_kernel, in_specs=[any_spec, pl.BlockSpec(memory_space=pltpu.VMEM)], out_specs=any_spec,
        out_shape=jax.ShapeDtypeStruct((n_tok, width), jnp.bfloat16), name='final_norm',
        scratch_shapes=[pltpu.VMEM((n_part, rows, width), jnp.bfloat16), pltpu.VMEM((n_part, rows, width), jnp.bfloat16),
                        pltpu.SemaphoreType.DMA((n_part,)), pltpu.SemaphoreType.DMA((n_part,))],
        compiler_params=pltpu.CompilerParams(vmem_limit_bytes=66_000_000),
        cost_estimate=pl.CostEstimate(flops=6 * n_tok * width, bytes_accessed=4 * n_tok * width, transcendentals=n_tok),
    )(h, gain[None])


def run_layer(h0, cos, sin, gain_attn, gain_mlp, w_query, w_key, w_value, w_out, w_gate, w_up, w_down, n_dev, n_seq):
    n_tok, width = h0.shape
    rows, n_heads, head_dim = w_query.shape
    kv_heads = w_key.shape[1]
    seq_len = n_tok // n_seq
    ff = w_gate.shape[1]
    rows_b = w_down.shape[0]
    w_q, w_k, w_v = (w.reshape(rows, -1) for w in (w_query, w_key, w_value))
    n_a = (w_q.shape[1] + w_k.shape[1] + w_v.shape[1] + width) // (2 * COLS) + ff // COLS
    n_b = 2 * (width // COLS)
    chips = n_dev // 2
    any_spec = pl.BlockSpec(memory_space=pl.ANY)
    vmem_spec = pl.BlockSpec(memory_space=pltpu.VMEM)
    n_weights = n_dev * (n_a * rows * 2 * COLS + rows_b * width)
    operands = (h0, w_q, w_k, w_v, w_out, w_gate, w_up, w_down, cos, sin, gain_attn[None], gain_mlp[None])
    out, _, _ = pl.pallas_call(
        functools.partial(layer_kernel, (n_seq, seq_len, n_heads, kv_heads, head_dim)),
        out_shape=(
            jax.ShapeDtypeStruct((n_tok, width), jnp.bfloat16),
            jax.ShapeDtypeStruct((n_a, chips, 2, 2, rows, COLS), jnp.bfloat16),
            jax.ShapeDtypeStruct((n_b, chips, 2, 2, rows_b // 4, COLS), jnp.bfloat16),
        ),
        in_specs=[any_spec] * 8 + [vmem_spec] * (len(operands) - 8),
        out_specs=(any_spec,) * 3,
        scratch_shapes=[
            pltpu.VMEM((n_tok, width), jnp.bfloat16),
            pltpu.VMEM((n_tok, width), jnp.bfloat16),
            pltpu.VMEM((n_heads + 2 * kv_heads, n_tok, head_dim), jnp.bfloat16),
            pltpu.VMEM((2, n_tok, ff // 2), jnp.bfloat16),
            pltpu.VMEM((n_tok, COLS), jnp.float32),
            pltpu.VMEM((n_tok, head_dim), jnp.float32),
            pltpu.VMEM((n_tok, head_dim), jnp.float32),
            pltpu.VMEM((2, chips, 2, 2, rows, COLS), jnp.bfloat16),
            pltpu.VMEM((2, chips, 2, 2, rows_b // 4, COLS), jnp.bfloat16),
            pltpu.SemaphoreType.DMA((n_a, N_RECV)),
            pltpu.SemaphoreType.DMA((n_b, N_RECV)),
            pltpu.SemaphoreType.DMA((n_a,)),
            pltpu.SemaphoreType.DMA((n_b,)),
            pltpu.SemaphoreType.DMA((n_a,)),
            pltpu.SemaphoreType.DMA((n_b,)),
            pltpu.SemaphoreType.DMA((2,)),
            pltpu.SemaphoreType.DMA((2,)),
            pltpu.SemaphoreType.DMA((2,)),
        ],
        compiler_params=pltpu.CompilerParams(
            collective_id=0, has_side_effects=True, vmem_limit_bytes=66_000_000),
        cost_estimate=pl.CostEstimate(flops=2 * n_tok * n_weights, bytes_accessed=4 * n_weights, transcendentals=0),
        name='prefill_layer',
    )(*operands)
    return out


def solution(mesh):
    token_spec = P(('data', 'wg'))
    weight_spec = P(None, 'wg')
    whole_spec = P()
    in_specs = (token_spec, token_spec, whole_spec, whole_spec, weight_spec, weight_spec, weight_spec, weight_spec, weight_spec, weight_spec, weight_spec, whole_spec)
    n_dev = mesh.shape['wg']
    assert n_dev == 2 * RING * RING

    def local_forward(h0, positions, norm_attn, norm_mlp, w_query, w_key, w_value, w_out, w_gate, w_up, w_down, norm_final):
        cos, sin = rope_tables(positions, w_query.shape[-1])
        residual = h0.reshape(-1, h0.shape[-1])
        for l in range(w_query.shape[0]):
            residual = run_layer(residual, cos, sin, norm_attn[l], norm_mlp[l], w_query[l], w_key[l], w_value[l],
                                 w_out[l], w_gate[l], w_up[l], w_down[l], n_dev, h0.shape[0])
        return final_norm(residual, norm_final).reshape(h0.shape)

    return jax.shard_map(local_forward, mesh=mesh, in_specs=in_specs, out_specs=token_spec, check_vma=False)
```
